512 devices in a mesh: slab: 8 (over z), tile: 64 (over x, y, core).
Axes of the slice: x: 4, y: 8, z: 8, core: 2. Of those that a mesh axis runs over, the one named last changes fastest.
Arguments:
- voxel_grid: float32 [4, 128, 512, 256], P(None, 'slab', 'tile'), may hold values from -4 to 4
- first_moment: float32 [4, 128, 512, 256], P(None, 'slab', 'tile'), may hold values from -0.75 to 0.75
- second_moment: float32 [4, 128, 512, 256], P(None, 'slab', 'tile'), may hold values from 0.01 to 0.5
- pixel_index: int32 [262144], P('tile'), may hold values from 0 to 2047
- start_slab: int32 [262144], P('tile'), may hold values from 0 to 3
- ray_count: int32 [262144], P('tile'), may hold values from 32 to 80
- target: float32 [3, 262144], P(None, 'tile'), may hold values from 0 to 1
Outputs:
- new_grid: float32 [4, 128, 512, 256], P(None, 'slab', 'tile')
- new_first: float32 [4, 128, 512, 256], P(None, 'slab', 'tile')
- new_second: float32 [4, 128, 512, 256], P(None, 'slab', 'tile')
The draws below stay inside these ranges and needn't reach their ends.
All inputs are finite; a program needn't handle non-finite values.
Results may differ from the reference program's by a relative error of at most 0.0003.
Values sent between devices are 32-bit elements; how exact they have to be, the bound alone decides.
A program may use at most 128 MiB of HBM per device.

```python
import math
import jax
import jax.numpy as jnp
from jax import lax

CZ = 16
CX = 8
NY = 256
RAYS_DEV = 4096
STEP = 20
NZ = 128
NX = 512
RAYS = 262144
HALF_SLABS = 4
N_TILE = 64


def place_ends(result, rng, least, top_value):
    longest = result.shape.index(max(result.shape))
    spots = []
    for shift in (0, 1):
        where = [jax.random.randint(jax.random.fold_in(rng, axis), (), 0, length) for axis, length in enumerate(result.shape)]
        where[longest] = (where[longest] + shift) % result.shape[longest]
        spots.append(tuple(where))
    return result.at[spots[0]].set(least).at[spots[1]].set(top_value)


def block_levels(key, shape, pieces, least, top_value):
    loudness = 1.0
    for axis_at, blocks in pieces:
        draws = jax.random.uniform(jax.random.fold_in(jax.random.fold_in(key, 6), axis_at), (blocks,), jnp.float32, least / len(pieces), top_value / len(pieces))
        loudness = loudness * jnp.repeat(jnp.exp(draws), shape[axis_at] // blocks).reshape((-1,) + (1,) * (len(shape) - 1 - axis_at))
    return loudness


def bell_draw(key, dims, spread, reach, split=(), kind=jnp.bfloat16):
    array = spread * jax.random.normal(key, dims, jnp.float32)
    if split:
        array = array * block_levels(key, dims, split, -0.22, 0.18)
    return jnp.clip(array, -reach, reach).astype(kind)


def setup_inputs(seed: int = 0) -> dict:
    seeds = jax.random.split(jax.random.key(seed), 8)
    return {
        "voxel_grid": bell_draw(seeds[0], (4, NZ, NX, NY), 1.0, 4.0, ((1, 8), (2, 64)), jnp.float32),
        "first_moment": bell_draw(seeds[1], (4, NZ, NX, NY), 0.05, 0.75, ((1, 8), (2, 64)), jnp.float32),
        "second_moment": jnp.clip(jnp.exp(math.log(0.5) - 3.912023 * jax.random.uniform(seeds[2], (4, NZ, NX, NY), jnp.float32) ** block_levels(seeds[2], (4, NZ, NX, NY), ((1, 8), (2, 64)), -0.2, 0.2)), 0.01, 0.5),
        "pixel_index": place_ends(jax.random.randint(seeds[3], (RAYS,), 0, CX * NY), jax.random.fold_in(seeds[3], 1), 0, (CX * NY) - 1).astype(jnp.int32),
        "start_slab": place_ends(jax.random.randint(seeds[4], (RAYS,), 0, HALF_SLABS), jax.random.fold_in(seeds[4], 1), 0, HALF_SLABS - 1).astype(jnp.int32),
        "ray_count": place_ends(jax.random.randint(seeds[5], (RAYS,), NZ // 4, NZ // 2 + CZ + 1), jax.random.fold_in(seeds[5], 1), NZ // 4, (NZ // 2 + CZ + 1) - 1).astype(jnp.int32),
        "target": jnp.clip(1.0 * jax.random.uniform(seeds[6], (3, RAYS), jnp.float32) ** block_levels(seeds[6], (3, RAYS), ((1, 64),), -0.2, 0.2), 0.0, 1.0),
    }


RENDER_WEIGHT = 1000.0
TV_WEIGHT = 0.05
BACKGROUND = 1.0
STEP_SPAN = 4.0
CLIP_RMS = 0.25
LEARN_RATE = 0.02
BETA_ONE = 0.9
BETA_TWO = 0.99
EPSILON = 1e-08

def tile_loss(tile_grid, pixel_index, start_slab, ray_count, target):
    flat = tile_grid.reshape(4, NZ, CX * NY)
    samples = jnp.take(flat, pixel_index, axis=2)
    depth_pos = jnp.arange(NZ, dtype=jnp.int32)[:, None]
    first_cell = start_slab[None, :] * CZ
    inside = (depth_pos >= first_cell) & (depth_pos < first_cell + ray_count[None, :])
    optical = jnp.where(inside, jax.nn.softplus(samples[0]) * (STEP_SPAN / NZ), 0.0)
    running = jnp.cumsum(optical, axis=0)
    weights = jnp.exp(-(running - optical)) * (1.0 - jnp.exp(-optical))
    colors = jax.nn.sigmoid(samples[1:4])
    rendered = lax.optimization_barrier(jnp.sum(weights[None] * colors, axis=1)) + jnp.exp(-running[-1])[None] * BACKGROUND
    return 0.5 * RENDER_WEIGHT * jnp.sum((rendered - target) ** 2)

def reference(voxel_grid, first_moment, second_moment, pixel_index, start_slab, ray_count, target):
    tiles = voxel_grid.reshape(4, NZ, N_TILE, CX, NY).transpose(2, 0, 1, 3, 4)
    pixels = pixel_index.reshape(N_TILE, RAYS_DEV)
    starts = start_slab.reshape(N_TILE, RAYS_DEV)
    counts = ray_count.reshape(N_TILE, RAYS_DEV)
    targets = target.reshape(3, N_TILE, RAYS_DEV).transpose(1, 0, 2)

    def one_tile(inputs):
        return jax.grad(tile_loss)(*inputs)
    tile_grads = lax.map(one_tile, (tiles, pixels, starts, counts, targets))
    render_grad = tile_grads.transpose(1, 2, 0, 3, 4).reshape(4, NZ, NX, NY)
    smooth = jnp.zeros_like(voxel_grid)
    for axis_num in (1, 2, 3):
        step_diff = jnp.diff(voxel_grid, axis=axis_num)
        low_pad = [(0, 0)] * 4
        high_pad = [(0, 0)] * 4
        low_pad[axis_num] = (0, 1)
        high_pad[axis_num] = (1, 0)
        smooth = smooth + jnp.pad(-step_diff, low_pad) + jnp.pad(step_diff, high_pad)
    gradient = render_grad + 2.0 * TV_WEIGHT * smooth
    norm_value = jnp.sqrt(jnp.sum(gradient * gradient))
    limit = CLIP_RMS * math.sqrt(4.0 * NZ * NX * NY)
    clipped = gradient * (limit / jnp.maximum(norm_value, limit))
    new_first = BETA_ONE * first_moment + (1.0 - BETA_ONE) * clipped
    new_second = BETA_TWO * second_moment + (1.0 - BETA_TWO) * clipped * clipped
    first_hat = new_first / (1.0 - BETA_ONE ** STEP)
    second_hat = new_second / (1.0 - BETA_TWO ** STEP)
    new_grid = voxel_grid - LEARN_RATE * first_hat / (jnp.sqrt(second_hat) + EPSILON)
    return (new_grid, new_first, new_second)
```

```python
import functools
import math

import jax
import jax.numpy as jnp
from jax import lax
from jax.experimental import pallas as pl
from jax.experimental.pallas import tpu as pltpu
from jax.sharding import Mesh
from jax.sharding import PartitionSpec as P

STEP = 20
AXES = ("slab", "tile_0", "tile_1", "tile_2")
TILE = AXES[1:]

RENDER_WEIGHT = 1000.0
TV_WEIGHT = 0.05
BACKGROUND = 1.0
STEP_SPAN = 4.0
CLIP_RMS = 0.25
LEARN_RATE = 0.02
BETA_ONE = 0.9
BETA_TWO = 0.99
EPSILON = 1e-08

MESH_ID = pl.DeviceIdType.MESH
F32 = jnp.float32
BF16 = jnp.bfloat16
DEPTH = 16
ROWS = 8
WIDE = 256
KEYS = DEPTH * ROWS
CELLS = 4 * KEYS


def split_bf16(value):
    high = value.astype(BF16)
    return high, (value - high.astype(F32)).astype(BF16)


def sigmoid(value):
    return 1.0 / (1.0 + jnp.exp(-value))


def gradient_kernel(
    sizes,
    step_width,
    grid_hbm,
    pixel_hbm,
    start_hbm,
    count_hbm,
    target_hbm,
    grad_hbm,
    total_ref,
    grid,
    pixel,
    start,
    count,
    target,
    table,
    shade,
    clear,
    share,
    smooth,
    spread,
    grad,
    edge_low,
    edge_high,
    z_low,
    z_high,
    x_low,
    x_high,
    out_part,
    in_part,
    out_cot,
    in_cot,
    mine_a,
    sums_a,
    mine_b,
    sums_b,
    load_sem,
    store_sem,
    halo_send,
    halo_recv,
    part_send,
    part_recv,
    cot_send,
    cot_recv,
    a_send,
    a_recv,
    b_send,
    b_recv,
    ready,
):
    slabs, size_x, size_y, cores = sizes
    group = pixel.shape[1] // slabs
    slab = lax.axis_index("slab")
    at_x = lax.axis_index("tile_0")
    at_y = lax.axis_index("tile_1")
    core = lax.axis_index("tile_2")
    tiles = size_x * size_y * cores
    tile = (at_x * size_y + at_y) * cores + core

    def tile_device(index):
        return (slab, index // (size_y * cores), (index // cores) % size_y, index % cores)

    loads = [
        pltpu.make_async_copy(source, into, load_sem.at[k])
        for k, (source, into) in enumerate(
            (
                (grid_hbm, grid),
                (pixel_hbm, pixel),
                (start_hbm, start),
                (count_hbm, count),
                (target_hbm, target),
            )
        )
    ]
    for load in loads:
        load.start()

    barrier = pltpu.get_barrier_semaphore()
    greeted = 0
    for off in range(1, slabs):
        pl.semaphore_signal(
            barrier,
            inc=1,
            device_id=((slab + off) % slabs, at_x, at_y, core),
            device_id_type=MESH_ID,
        )
        greeted += 1
    for off in range(1, size_x):
        pl.semaphore_signal(
            barrier,
            inc=1,
            device_id=(slab, (at_x + off) % size_x, at_y, core),
            device_id_type=MESH_ID,
        )
        greeted += 1
    for off in range(1, size_y):
        pl.semaphore_signal(
            barrier,
            inc=1,
            device_id=(slab, at_x, (at_y + off) % size_y, core),
            device_id_type=MESH_ID,
        )
        greeted += 1
    for off in (1, tiles - 1):
        pl.semaphore_signal(
            barrier,
            inc=1,
            device_id=tile_device((tile + off) % tiles),
            device_id_type=MESH_ID,
        )
        greeted += 1

    loads[0].wait()
    light = jnp.ones((ROWS, WIDE), F32)
    color = [jnp.zeros((ROWS, WIDE), F32) for _ in range(3)]
    pairs = []
    for z in range(DEPTH):
        raw = grid[pl.ds(z * ROWS, ROWS), :]
        soft = jnp.maximum(raw, 0.0) + jnp.log(1.0 + jnp.exp(-jnp.abs(raw)))
        stay = jnp.exp(-(soft * step_width))
        weight = light * (1.0 - stay)
        light = light * stay
        share[pl.ds(z * ROWS, ROWS), :] = weight
        clear[pl.ds(z * ROWS, ROWS), :] = light
        for c in range(3):
            tone = sigmoid(grid[pl.ds((c + 1) * KEYS + z * ROWS, ROWS), :])
            shade[pl.ds(c * KEYS + z * ROWS, ROWS), :] = tone
            color[c] = color[c] + weight * tone
        pairs.append((*color, 1.0 - light))
        if z % 2:
            for c in range(4):
                high, low = split_bf16(jnp.concatenate([pairs[-2][c], pairs[-1][c]], axis=0))
                rows = pl.ds(c * KEYS + (z - 1) * ROWS, 2 * ROWS)
                table[rows, pl.ds(0, WIDE)] = high
                table[rows, pl.ds(WIDE, WIDE)] = low
    for load in loads[1:]:
        load.wait()

    def partner(place):
        half = (place + 1) // 2
        return (slab + half * (2 * (place % 2) - 1) + slabs) % slabs

    def rays_of(other):
        lanes = pl.ds(pl.multiple_of(other * group, group), group)
        cell = pixel[:, lanes]
        begin = start[:, lanes]
        taken = begin * DEPTH + count[:, lanes] - slab * DEPTH
        taken = jnp.where(begin <= slab, jnp.clip(taken, 0, DEPTH), 0)
        key = (taken - 1) * ROWS + cell // WIDE
        across = lax.broadcasted_iota(jnp.int32, (WIDE, group), 0)
        column = jnp.where(across == cell % WIDE, 1.0, 0.0).astype(BF16)
        return key, column

    def part_copy(other):
        return pltpu.make_async_remote_copy(
            src_ref=out_part.at[other],
            dst_ref=in_part.at[slab],
            send_sem=part_send.at[other],
            recv_sem=part_recv.at[slab],
            device_id=(other, at_x, at_y, core),
            device_id_type=MESH_ID,
        )

    def part_arrival(other):
        return pltpu.make_async_remote_copy(
            src_ref=out_part.at[other],
            dst_ref=in_part.at[other],
            send_sem=part_send.at[other],
            recv_sem=part_recv.at[other],
            device_id=(other, at_x, at_y, core),
            device_id_type=MESH_ID,
        )

    def look_up(other):
        key, column = rays_of(other)
        found = jnp.dot(
            table[...],
            jnp.concatenate([column, column], axis=0),
            preferred_element_type=F32,
        )
        chosen = lax.broadcasted_iota(jnp.int32, (KEYS, group), 0) == key
        values = [
            jnp.sum(
                jnp.where(chosen, found[c * KEYS : (c + 1) * KEYS], 0.0),
                axis=0,
                keepdims=True,
            )
            for c in range(4)
        ]
        values[3] = 1.0 - values[3]
        return jnp.concatenate(values, axis=0)

    def look_up_and_send(order, carry):
        other = partner(slabs - 1 - order)
        out_part[other] = look_up(other)

        @pl.when(order == 0)
        def _():
            pl.semaphore_wait(barrier, greeted)

        part_copy(other).start()
        return carry

    lax.fori_loop(0, slabs - 1, look_up_and_send, 0)
    in_part[slab] = look_up(slab)

    for off in range(1, size_y):
        pl.semaphore_signal(
            ready,
            inc=1,
            device_id=(slab, at_x, (at_y + off) % size_y, core),
            device_id_type=MESH_ID,
        )
    for k in range(CELLS // ROWS):
        edge_low[pl.ds(k, 1), :] = grid[pl.ds(k * ROWS, 1), :]
        edge_high[pl.ds(k, 1), :] = grid[pl.ds(k * ROWS + ROWS - 1, 1), :]
    next_slab = ((slab + 1) % slabs, at_x, at_y, core)
    prev_slab = ((slab + slabs - 1) % slabs, at_x, at_y, core)
    next_tile = tile_device((tile + 1) % tiles)
    prev_tile = tile_device((tile + tiles - 1) % tiles)
    halos = []
    for c in range(4):
        last = grid.at[pl.ds(c * KEYS + (DEPTH - 1) * ROWS, ROWS)]
        first = grid.at[pl.ds(c * KEYS, ROWS)]
        halos.append((last, z_low.at[c], next_slab))
        halos.append((first, z_high.at[c], prev_slab))
    halos.append((edge_high, x_low, next_tile))
    halos.append((edge_low, x_high, prev_tile))
    halos = [
        pltpu.make_async_remote_copy(
            src_ref=source,
            dst_ref=into,
            send_sem=halo_send.at[k],
            recv_sem=halo_recv.at[k],
            device_id=device,
            device_id_type=MESH_ID,
        )
        for k, (source, into, device) in enumerate(halos)
    ]
    for halo in halos:
        halo.start()
    for halo in halos:
        halo.wait()

    row_at = lax.broadcasted_iota(jnp.int32, (ROWS, WIDE), 0)
    lane_at = lax.broadcasted_iota(jnp.int32, (ROWS, WIDE), 1)

    def smooth_channel(c, carry):
        base = c * KEYS
        for z in range(DEPTH):
            here = pl.ds(pl.multiple_of(base + z * ROWS, ROWS), ROWS)
            value = grid[here, :]
            if z > 0:
                total = value - grid[pl.ds(pl.multiple_of(base + (z - 1) * ROWS, ROWS), ROWS), :]
            else:
                total = jnp.where(slab > 0, value - z_low[c], 0.0)
            if z < DEPTH - 1:
                total += value - grid[pl.ds(pl.multiple_of(base + (z + 1) * ROWS, ROWS), ROWS), :]
            else:
                total += jnp.where(slab < slabs - 1, value - z_high[c], 0.0)
            below = jnp.where(
                row_at == 0, x_low[pl.ds(c * DEPTH + z, 1), :], pltpu.roll(value, 1, 0)
            )
            above = jnp.where(
                row_at == ROWS - 1,
                x_high[pl.ds(c * DEPTH + z, 1), :],
                pltpu.roll(value, ROWS - 1, 0),
            )
            total += jnp.where((row_at > 0) | (tile > 0), value - below, 0.0)
            total += jnp.where((row_at < ROWS - 1) | (tile < tiles - 1), value - above, 0.0)
            total += jnp.where(lane_at > 0, value - pltpu.roll(value, 1, 1), 0.0)
            total += jnp.where(lane_at < WIDE - 1, value - pltpu.roll(value, WIDE - 1, 1), 0.0)
            smooth[here, :] = (2.0 * TV_WEIGHT) * total
        return carry

    lax.fori_loop(0, 4, smooth_channel, 0)

    def await_part(order, carry):
        part_arrival(partner(order)).wait_recv()
        return carry

    lax.fori_loop(1, slabs, await_part, 0)
    goal = target[:, pl.ds(pl.multiple_of(slab * group, group), group)]
    ahead = jnp.ones((1, group), F32)
    rendered = jnp.zeros((3, group), F32)
    reach = []
    for s in range(slabs):
        reach.append(ahead)
        part = in_part[s]
        rendered = rendered + ahead * part[:3]
        ahead = ahead * part[3:]
    residual = RENDER_WEIGHT * (rendered + ahead * BACKGROUND - goal)
    beyond = jnp.full((3, group), BACKGROUND, F32)
    for s in range(slabs - 1, -1, -1):
        product = residual * beyond
        dark = product[0:1] + product[1:2] + product[2:3]
        out_cot[s] = reach[s] * jnp.concatenate([residual, dark], axis=0)
        part = in_part[s]
        beyond = part[:3] + part[3:] * beyond

    def cot_copy(other):
        return pltpu.make_async_remote_copy(
            src_ref=out_cot.at[other],
            dst_ref=in_cot.at[slab],
            send_sem=cot_send.at[other],
            recv_sem=cot_recv.at[slab],
            device_id=(other, at_x, at_y, core),
            device_id_type=MESH_ID,
        )

    def cot_arrival(other):
        return pltpu.make_async_remote_copy(
            src_ref=out_cot.at[other],
            dst_ref=in_cot.at[other],
            send_sem=cot_send.at[other],
            recv_sem=cot_recv.at[other],
            device_id=(other, at_x, at_y, core),
            device_id_type=MESH_ID,
        )

    def send_cot(order, carry):
        cot_copy(partner(slabs - 1 - order)).start()
        return carry

    lax.fori_loop(0, slabs - 1, send_cot, 0)
    in_cot[slab] = out_cot[slab]
    spread[...] = jnp.zeros_like(spread)

    def scatter(order, carry):
        other = partner(order)

        @pl.when(order > 0)
        def _():
            cot_arrival(other).wait_recv()

        key, column = rays_of(other)
        chosen = jnp.where(
            lax.broadcasted_iota(jnp.int32, (KEYS, group), 0) == key, 1.0, 0.0
        ).astype(BF16)
        cot = in_cot[other]
        high, low = split_bf16(cot)
        left = jnp.concatenate(
            [
                jnp.concatenate([chosen * high[c : c + 1], chosen * low[c : c + 1]], axis=1)
                for c in range(4)
            ],
            axis=0,
        )
        spread[...] += lax.dot_general(
            left,
            jnp.concatenate([column, column], axis=1),
            (((1,), (1,)), ((), ())),
            preferred_element_type=F32,
        )
        return carry

    lax.fori_loop(0, slabs, scatter, 0)

    later = [jnp.zeros((ROWS, WIDE), F32) for _ in range(3)]
    tail = jnp.zeros((ROWS, WIDE), F32)
    squares = jnp.zeros((ROWS, WIDE), F32)
    for z in range(DEPTH - 1, -1, -1):
        here = pl.ds(z * ROWS, ROWS)
        weight = share[here, :]
        light = clear[here, :]
        pull = jnp.zeros((ROWS, WIDE), F32)
        for c in range(3):
            rows = pl.ds(c * KEYS + z * ROWS, ROWS)
            tone = shade[rows, :]
            later[c] = later[c] + spread[rows, :]
            pull = pull + tone * later[c]
            rows = pl.ds((c + 1) * KEYS + z * ROWS, ROWS)
            value = weight * later[c] * (tone * (1.0 - tone)) + smooth[rows, :]
            grad[rows, :] = value
            squares = squares + value * value
        tail = tail + spread[pl.ds(3 * KEYS + z * ROWS, ROWS), :] * light
        thick = pull * light - tail
        tail = tail + pull * weight
        value = thick * (step_width * sigmoid(grid[here, :])) + smooth[here, :]
        grad[here, :] = value
        squares = squares + value * value
    out_copy = pltpu.make_async_copy(grad, grad_hbm, store_sem)
    out_copy.start()

    squares = squares[:, :128] + squares[:, 128:]
    own = jnp.sum(squares, axis=0, keepdims=True)
    mine_a[...] = own
    n_a = slabs * cores
    me_a = slab * cores + core

    def a_copy(off, slot):
        to = (me_a + off) % n_a
        return pltpu.make_async_remote_copy(
            src_ref=mine_a,
            dst_ref=sums_a.at[slot],
            send_sem=a_send.at[off],
            recv_sem=a_recv.at[slot],
            device_id=(to // cores, at_x, at_y, to % cores),
            device_id_type=MESH_ID,
        )

    def each(first, last, do):
        def body(k, carry):
            do(k)
            return carry

        lax.fori_loop(first, last, body, 0)

    each(1, n_a, lambda off: a_copy(off, me_a).start())
    sums_a[me_a] = own
    each(1, n_a, lambda off: a_copy(off, (me_a + off) % n_a).wait_recv())
    own = jnp.sum(sums_a[...], axis=0)
    mine_b[...] = own
    n_b = size_x * size_y
    me_b = at_x * size_y + at_y

    def b_copy(off, slot):
        to = (me_b + off) % n_b
        return pltpu.make_async_remote_copy(
            src_ref=mine_b,
            dst_ref=sums_b.at[slot],
            send_sem=b_send.at[off],
            recv_sem=b_recv.at[slot],
            device_id=(slab, to // size_y, to % size_y, core),
            device_id_type=MESH_ID,
        )

    if size_y > 1:
        pl.semaphore_wait(ready, size_y - 1)
    each(1, n_b, lambda off: b_copy(off, me_b).start())
    sums_b[me_b] = own
    each(1, n_b, lambda off: b_copy(off, (me_b + off) % n_b).wait_recv())
    total_ref[...] = jnp.sum(sums_b[...], axis=0)

    each(1, slabs, lambda k: part_copy(partner(k)).wait_send())
    each(1, slabs, lambda k: cot_copy(partner(k)).wait_send())
    each(1, n_a, lambda off: a_copy(off, me_a).wait_send())
    each(1, n_b, lambda off: b_copy(off, me_b).wait_send())
    out_copy.wait()


def update_kernel(limit, grid_ref, first_ref, second_ref, grad_ref, total_ref, *outs):
    new_grid, new_first, new_second = outs
    norm = jnp.sqrt(jnp.sum(total_ref[...], axis=1, keepdims=True))
    scale = limit / jnp.maximum(norm, limit)
    clipped = grad_ref[...] * scale
    first = BETA_ONE * first_ref[...] + (1.0 - BETA_ONE) * clipped
    second = BETA_TWO * second_ref[...] + (1.0 - BETA_TWO) * clipped * clipped
    new_first[...] = first
    new_second[...] = second
    first_hat = first * (1.0 / (1.0 - BETA_ONE**STEP))
    second_hat = second * (1.0 / (1.0 - BETA_TWO**STEP))
    new_grid[...] = grid_ref[...] - LEARN_RATE * first_hat / (jnp.sqrt(second_hat) + EPSILON)


def per_device(voxel_grid, first_moment, second_moment, pixel_index, start_slab, ray_count, target):
    sizes = tuple(lax.axis_size(axis) for axis in AXES)
    slabs = sizes[0]
    rays = pixel_index.shape[0]
    group = rays // slabs
    total_depth = DEPTH * slabs
    total_x = ROWS * math.prod(sizes[1:])
    n_a = slabs * sizes[3]
    n_b = sizes[1] * sizes[2]
    flat = (CELLS, WIDE)
    dma = pltpu.SemaphoreType.DMA
    anywhere = pl.BlockSpec(memory_space=pl.ANY)
    grad, total = pl.pallas_call(
        functools.partial(gradient_kernel, sizes, STEP_SPAN / total_depth),
        out_shape=(
            jax.ShapeDtypeStruct(flat, F32),
            jax.ShapeDtypeStruct((1, 128), F32),
        ),
        in_specs=[anywhere] * 5,
        out_specs=(anywhere, pl.BlockSpec(memory_space=pltpu.VMEM)),
        scratch_shapes=[
            pltpu.VMEM(flat, F32),
            pltpu.VMEM((1, rays), jnp.int32),
            pltpu.VMEM((1, rays), jnp.int32),
            pltpu.VMEM((1, rays), jnp.int32),
            pltpu.VMEM((3, rays), F32),
            pltpu.VMEM((CELLS, 2 * WIDE), BF16),
            pltpu.VMEM((3 * KEYS, WIDE), F32),
            pltpu.VMEM((KEYS, WIDE), F32),
            pltpu.VMEM((KEYS, WIDE), F32),
            pltpu.VMEM(flat, F32),
            pltpu.VMEM(flat, F32),
            pltpu.VMEM(flat, F32),
            pltpu.VMEM((CELLS // ROWS, WIDE), F32),
            pltpu.VMEM((CELLS // ROWS, WIDE), F32),
            pltpu.VMEM((4, ROWS, WIDE), F32),
            pltpu.VMEM((4, ROWS, WIDE), F32),
            pltpu.VMEM((CELLS // ROWS, WIDE), F32),
            pltpu.VMEM((CELLS // ROWS, WIDE), F32),
            pltpu.VMEM((slabs, 4, group), F32),
            pltpu.VMEM((slabs, 4, group), F32),
            pltpu.VMEM((slabs, 4, group), F32),
            pltpu.VMEM((slabs, 4, group), F32),
            pltpu.VMEM((1, 128), F32),
            pltpu.VMEM((n_a, 1, 128), F32),
            pltpu.VMEM((1, 128), F32),
            pltpu.VMEM((n_b, 1, 128), F32),
            dma((5,)),
            dma,
            dma((10,)),
            dma((10,)),
            dma((slabs,)),
            dma((slabs,)),
            dma((slabs,)),
            dma((slabs,)),
            dma((n_a,)),
            dma((n_a,)),
            dma((n_b,)),
            dma((n_b,)),
            pltpu.SemaphoreType.REGULAR,
        ],
        compiler_params=pltpu.CompilerParams(collective_id=0, has_side_effects=True),
        name="render_gradient",
    )(
        voxel_grid.reshape(flat),
        pixel_index.reshape(1, rays),
        start_slab.reshape(1, rays),
        ray_count.reshape(1, rays),
        target,
    )
    limit = CLIP_RMS * math.sqrt(4.0 * total_depth * total_x * WIDE)
    block = pl.BlockSpec((KEYS, WIDE), lambda i: (i, 0))
    outs = pl.pallas_call(
        functools.partial(update_kernel, limit),
        grid=(4,),
        out_shape=[jax.ShapeDtypeStruct(flat, F32)] * 3,
        in_specs=[block] * 4 + [pl.BlockSpec((1, 128), lambda i: (0, 0))],
        out_specs=[block] * 3,
        name="clipped_adam",
    )(
        voxel_grid.reshape(flat),
        first_moment.reshape(flat),
        second_moment.reshape(flat),
        grad,
        total,
    )
    return tuple(out.reshape(voxel_grid.shape) for out in outs)


def solution(mesh):
    torus = Mesh(mesh.devices.reshape(mesh.shape["slab"], 4, 8, 2), AXES)
    cells = P(None, "slab", TILE, None)
    rays = P(TILE)
    return jax.shard_map(
        per_device,
        mesh=torus,
        in_specs=(cells, cells, cells, rays, rays, rays, P(None, TILE)),
        out_specs=(cells, cells, cells),
        check_vma=False,
    )
```

```python
import functools
import math

import jax
import jax.numpy as jnp
from jax import lax
from jax.experimental import pallas as pl
from jax.experimental.pallas import tpu as pltpu
from jax.sharding import Mesh
from jax.sharding import PartitionSpec as P

STEP = 20
AXES = ("slab", "tile_0", "tile_1", "tile_2")
TILE = AXES[1:]

RENDER_WEIGHT = 1000.0
TV_WEIGHT = 0.05
BACKGROUND = 1.0
STEP_SPAN = 4.0
CLIP_RMS = 0.25
LEARN_RATE = 0.02
BETA_ONE = 0.9
BETA_TWO = 0.99
EPSILON = 1e-08

MESH_ID = pl.DeviceIdType.MESH
F32 = jnp.float32
BF16 = jnp.bfloat16
DEPTH = 16
ROWS = 8
WIDE = 256
KEYS = DEPTH * ROWS
CELLS = 4 * KEYS


def split_bf16(value):
    high = value.astype(BF16)
    return high, (value - high.astype(F32)).astype(BF16)


def sigmoid(value):
    return 1.0 / (1.0 + jnp.exp(-value))


def gradient_kernel(
    sizes,
    step_width,
    grid_hbm,
    first_hbm,
    second_hbm,
    pixel_hbm,
    start_hbm,
    count_hbm,
    target_hbm,
    grid,
    first,
    second,
    grad,
    total_ref,
    pixel,
    start,
    count,
    target,
    table,
    shade,
    clear,
    share,
    smooth,
    spread,
    columns,
    chosens,
    edges,
    halo,
    out_part,
    in_part,
    out_cot,
    in_cot,
    mine,
    sums_a,
    sums_b,
    grid_sem,
    rays_sem,
    moment_sem,
    halo_sem,
    part_sem,
    cot_send,
    cot_recv,
    a_sem,
    b_sem,
    ready,
):
    slabs, size_x, size_y, cores = sizes
    group = pixel.shape[1] // slabs
    slab = lax.axis_index("slab")
    at_x = lax.axis_index("tile_0")
    at_y = lax.axis_index("tile_1")
    core = lax.axis_index("tile_2")
    tiles = size_x * size_y * cores
    tile = (at_x * size_y + at_y) * cores + core
    n_a = slabs * cores
    n_b = size_x * size_y

    def remote(source, into, send, recv, device):
        return pltpu.make_async_remote_copy(
            src_ref=source,
            dst_ref=into,
            send_sem=send,
            recv_sem=recv,
            device_id=device,
            device_id_type=MESH_ID,
        )

    def signal(semaphore, device):
        pl.semaphore_signal(semaphore, inc=1, device_id=device, device_id_type=MESH_ID)

    def tile_device(index):
        return (slab, index // (size_y * cores), (index // cores) % size_y, index % cores)

    def far_first(size):
        return sorted(range(1, size), key=lambda off: -min(off, size - off))

    over_a = [(z, c) for z in far_first(slabs) + [0] for c in range(cores) if z or c]
    over_b = sorted(
        ((x, y) for x in range(size_x) for y in range(size_y) if x or y),
        key=lambda off: -min(off[0], size_x - off[0]) - min(off[1], size_y - off[1]),
    )

    def device_a(off):
        return ((slab + off[0]) % slabs, at_x, at_y, (core + off[1]) % cores)

    def device_b(off):
        return (slab, (at_x + off[0]) % size_x, (at_y + off[1]) % size_y, core)

    barrier = pltpu.get_barrier_semaphore()
    greet = [device_a(off) for off in over_a]
    greet += [device_b((0, y)) for y in far_first(size_y)]
    greet += [device_b((x, 0)) for x in far_first(size_x)]
    next_tile = tile_device((tile + 1) % tiles)
    prev_tile = tile_device((tile + tiles - 1) % tiles)
    greet += [next_tile, prev_tile]

    load_grid = pltpu.make_async_copy(grid_hbm, grid, grid_sem)
    load_grid.start()
    for device in greet:
        signal(barrier, device)
    ray_loads = [
        pltpu.make_async_copy(source, into, rays_sem.at[k])
        for k, (source, into) in enumerate(
            ((pixel_hbm, pixel), (start_hbm, start), (count_hbm, count), (target_hbm, target))
        )
    ]
    for load in ray_loads:
        load.start()
    moment_loads = [
        pltpu.make_async_copy(first_hbm, first, moment_sem.at[0]),
        pltpu.make_async_copy(second_hbm, second, moment_sem.at[1]),
    ]
    for load in moment_loads:
        load.start()

    load_grid.wait()
    light = jnp.ones((ROWS, WIDE), F32)
    color = [jnp.zeros((ROWS, WIDE), F32) for _ in range(3)]
    pairs = []
    for z in range(DEPTH):
        raw = grid[0, z]
        soft = jnp.maximum(raw, 0.0) + jnp.log(1.0 + jnp.exp(-jnp.abs(raw)))
        stay = jnp.exp(-(soft * step_width))
        weight = light * (1.0 - stay)
        light = light * stay
        share[z] = weight
        clear[z] = light
        for c in range(3):
            tone = sigmoid(grid[c + 1, z])
            shade[c, z] = tone
            color[c] = color[c] + weight * tone
        pairs.append((*color, 1.0 - light))
        if z % 2:
            for c in range(4):
                high, low = split_bf16(jnp.concatenate([pairs[-2][c], pairs[-1][c]], axis=0))
                rows = pl.ds(c * KEYS + (z - 1) * ROWS, 2 * ROWS)
                table[rows, pl.ds(0, WIDE)] = high
                table[rows, pl.ds(WIDE, WIDE)] = low
    for load in ray_loads:
        load.wait()

    def partner(place):
        half = (place + 1) // 2
        return (slab + half * (2 * (place % 2) - 1) + slabs) % slabs

    def ring(other):
        return (other, at_x, at_y, core)

    def look_up(other):
        lanes = pl.ds(pl.multiple_of(other * group, group), group)
        cell = pixel[:, lanes]
        begin = start[:, lanes]
        taken = begin * DEPTH + count[:, lanes] - slab * DEPTH
        taken = jnp.where(begin <= slab, jnp.clip(taken, 0, DEPTH), 0)
        key = (taken - 1) * ROWS + cell // WIDE
        across = lax.broadcasted_iota(jnp.int32, (WIDE, group), 0)
        column = jnp.where(across == cell % WIDE, 1.0, 0.0).astype(BF16)
        columns[other] = column
        found = jnp.dot(
            table[...],
            jnp.concatenate([column, column], axis=0),
            preferred_element_type=F32,
        )
        chosen = lax.broadcasted_iota(jnp.int32, (KEYS, group), 0) == key
        chosens[other] = jnp.where(chosen, 1.0, 0.0).astype(BF16)
        values = [
            jnp.sum(
                jnp.where(chosen, found[c * KEYS : (c + 1) * KEYS], 0.0),
                axis=0,
                keepdims=True,
            )
            for c in range(4)
        ]
        values[3] = 1.0 - values[3]
        return jnp.concatenate(values, axis=0)

    def send_part(other):
        remote(
            out_part.at[other], in_part.at[slab], part_sem.at[0], part_sem.at[1], ring(other)
        ).start()

    places = list(range(slabs - 1, 0, -1))
    early = places[: slabs // 2]
    for place in early:
        out_part[partner(place)] = look_up(partner(place))
    pl.semaphore_wait(barrier, len(greet))
    for place in early:
        send_part(partner(place))
    for place in places[slabs // 2 :]:
        out_part[partner(place)] = look_up(partner(place))
        send_part(partner(place))
    in_part[slab] = look_up(slab)

    for off in far_first(size_y):
        signal(ready, device_b((0, off)))
    for c in range(4):
        for z in range(DEPTH):
            k = c * DEPTH + z
            edges[0, k // ROWS, pl.ds(k % ROWS, 1), :] = grid[c, z, pl.ds(ROWS - 1, 1), :]
            edges[1, k // ROWS, pl.ds(k % ROWS, 1), :] = grid[c, z, pl.ds(0, 1), :]
    for source, into, device in (
        (edges.at[0], halo.at[pl.ds(8, 8)], next_tile),
        (edges.at[1], halo.at[pl.ds(16, 8)], prev_tile),
        (grid.at[:, DEPTH - 1], halo.at[pl.ds(0, 4)], device_a((1, 0))),
        (grid.at[:, 0], halo.at[pl.ds(4, 4)], device_a((slabs - 1, 0))),
    ):
        remote(source, into, halo_sem.at[0], halo_sem.at[1], device).start()

    others = pl.ds(0, slabs - 1)
    all_parts = remote(
        out_part.at[others], in_part.at[others], part_sem.at[0], part_sem.at[1], ring(slab)
    )
    goal = target[:, pl.ds(pl.multiple_of(slab * group, group), group)]
    all_parts.wait_recv()
    ahead = jnp.ones((1, group), F32)
    rendered = jnp.zeros((3, group), F32)
    reach = []
    for s in range(slabs):
        reach.append(ahead)
        part = in_part[s]
        rendered = rendered + ahead * part[:3]
        ahead = ahead * part[3:]
    residual = RENDER_WEIGHT * (rendered + ahead * BACKGROUND - goal)
    beyond = jnp.full((3, group), BACKGROUND, F32)
    for s in range(slabs - 1, -1, -1):
        product = residual * beyond
        dark = product[0:1] + product[1:2] + product[2:3]
        out_cot[s] = reach[s] * jnp.concatenate([residual, dark], axis=0)
        part = in_part[s]
        beyond = part[:3] + part[3:] * beyond

    for place in places:
        other = partner(place)
        remote(
            out_cot.at[other], in_cot.at[slab], cot_send, cot_recv.at[slab], ring(other)
        ).start()

    def scatter(other, cot):
        high, low = split_bf16(cot)
        chosen = chosens[other]
        column = columns[other]
        left = jnp.concatenate(
            [
                jnp.concatenate([chosen * high[c : c + 1], chosen * low[c : c + 1]], axis=1)
                for c in range(4)
            ],
            axis=0,
        )
        return lax.dot_general(
            left,
            jnp.concatenate([column, column], axis=1),
            (((1,), (1,)), ((), ())),
            preferred_element_type=F32,
        )

    spread[...] = scatter(slab, out_cot[slab])

    remote(halo, halo, halo_sem.at[0], halo_sem.at[1], next_tile).wait()
    row_at = lax.broadcasted_iota(jnp.int32, (ROWS, WIDE), 0)
    lane_at = lax.broadcasted_iota(jnp.int32, (ROWS, WIDE), 1)

    def smooth_channel(c, carry):
        for z in range(DEPTH):
            value = grid[c, z]
            if z > 0:
                total = value - grid[c, z - 1]
            else:
                total = jnp.where(slab > 0, value - halo[c], 0.0)
            if z < DEPTH - 1:
                total += value - grid[c, z + 1]
            else:
                total += jnp.where(slab < slabs - 1, value - halo[4 + c], 0.0)
            line = (2 * c + z // ROWS, pl.ds(z % ROWS, 1), slice(None))
            below = jnp.where(
                row_at == 0, halo[8 + line[0], line[1], line[2]], pltpu.roll(value, 1, 0)
            )
            above = jnp.where(
                row_at == ROWS - 1,
                halo[16 + line[0], line[1], line[2]],
                pltpu.roll(value, ROWS - 1, 0),
            )
            total += jnp.where((row_at > 0) | (tile > 0), value - below, 0.0)
            total += jnp.where((row_at < ROWS - 1) | (tile < tiles - 1), value - above, 0.0)
            total += jnp.where(lane_at > 0, value - pltpu.roll(value, 1, 1), 0.0)
            total += jnp.where(lane_at < WIDE - 1, value - pltpu.roll(value, WIDE - 1, 1), 0.0)
            smooth[c, z] = (2.0 * TV_WEIGHT) * total
        return carry

    lax.fori_loop(0, 4, smooth_channel, 0)

    def scatter_arrived(place, carry):
        other = partner(place)
        remote(
            out_cot.at[other], in_cot.at[other], cot_send, cot_recv.at[other], ring(other)
        ).wait_recv()
        spread[...] += scatter(other, in_cot[other])
        return carry

    lax.fori_loop(1, slabs, scatter_arrived, 0)

    later = [jnp.zeros((ROWS, WIDE), F32) for _ in range(3)]
    tail = jnp.zeros((ROWS, WIDE), F32)
    squares = jnp.zeros((ROWS, WIDE), F32)
    for z in range(DEPTH - 1, -1, -1):
        weight = share[z]
        light = clear[z]
        pull = jnp.zeros((ROWS, WIDE), F32)
        for c in range(3):
            tone = shade[c, z]
            later[c] = later[c] + spread[pl.ds(c * KEYS + z * ROWS, ROWS), :]
            pull = pull + tone * later[c]
            value = weight * later[c] * (tone * (1.0 - tone)) + smooth[c + 1, z]
            grad[c + 1, z] = value
            squares = squares + value * value
        tail = tail + spread[pl.ds(3 * KEYS + z * ROWS, ROWS), :] * light
        thick = pull * light - tail
        tail = tail + pull * weight
        value = thick * (step_width * sigmoid(grid[0, z])) + smooth[0, z]
        grad[0, z] = value
        squares = squares + value * value

    squares = squares[:, :128] + squares[:, 128:]
    own = jnp.sum(squares, axis=0, keepdims=True)
    mine[0] = own
    me_a = slab * cores + core
    for off in over_a:
        remote(mine.at[0], sums_a.at[me_a], a_sem.at[0], a_sem.at[1], device_a(off)).start()
    sums_a[me_a] = own
    all_parts.wait_send()
    remote(
        out_cot.at[others], in_cot.at[others], cot_send, cot_recv.at[0], ring(slab)
    ).wait_send()
    for load in moment_loads:
        load.wait()
    if size_y > 1:
        pl.semaphore_wait(ready, size_y - 1)
    some = sums_a.at[pl.ds(0, n_a - 1)]
    remote(some, some, a_sem.at[0], a_sem.at[1], next_tile).wait()
    own = jnp.sum(sums_a[...], axis=0)
    mine[1] = own
    me_b = at_x * size_y + at_y
    for off in over_b:
        remote(mine.at[1], sums_b.at[me_b], b_sem.at[0], b_sem.at[1], device_b(off)).start()
    sums_b[me_b] = own
    some = sums_b.at[pl.ds(0, n_b - 1)]
    remote(some, some, b_sem.at[0], b_sem.at[1], next_tile).wait()
    total_ref[...] = jnp.sum(sums_b[...], axis=0)


def update_kernel(limit, grid, first, second, grad, total, *rest):
    outs, held, sem = rest[:3], rest[3:6], rest[6]
    norm = jnp.sqrt(jnp.sum(total[...], axis=1, keepdims=True))
    scale = limit / jnp.maximum(norm, limit)
    for c in range(4):
        clipped = grad[c] * scale
        new_first = BETA_ONE * first[c] + (1.0 - BETA_ONE) * clipped
        new_second = BETA_TWO * second[c] + (1.0 - BETA_TWO) * clipped * clipped
        held[1][c] = new_first
        held[2][c] = new_second
        first_hat = new_first * (1.0 / (1.0 - BETA_ONE**STEP))
        second_hat = new_second * (1.0 / (1.0 - BETA_TWO**STEP))
        held[0][c] = grid[c] - LEARN_RATE * first_hat / (jnp.sqrt(second_hat) + EPSILON)
        for k in range(3):
            pltpu.make_async_copy(held[k].at[c], outs[k].at[c], sem.at[k]).start()
    for k in range(3):
        pltpu.make_async_copy(held[k], outs[k], sem.at[k]).wait()


def per_device(voxel_grid, first_moment, second_moment, pixel_index, start_slab, ray_count, target):
    sizes = tuple(lax.axis_size(axis) for axis in AXES)
    slabs = sizes[0]
    rays = pixel_index.shape[0]
    group = rays // slabs
    total_depth = DEPTH * slabs
    total_x = ROWS * math.prod(sizes[1:])
    n_a = slabs * sizes[3]
    n_b = sizes[1] * sizes[2]
    block = (4, DEPTH, ROWS, WIDE)
    dma = pltpu.SemaphoreType.DMA
    anywhere = pl.BlockSpec(memory_space=pl.ANY)
    inside = pl.BlockSpec(memory_space=pltpu.VMEM)
    held = pltpu.VMEM(block, F32)
    grid, first, second, grad, total = pl.pallas_call(
        functools.partial(gradient_kernel, sizes, STEP_SPAN / total_depth),
        out_shape=(held, held, held, held, pltpu.VMEM((1, 128), F32)),
        in_specs=[anywhere] * 7,
        out_specs=(inside,) * 5,
        scratch_shapes=[
            pltpu.VMEM((1, rays), jnp.int32),
            pltpu.VMEM((1, rays), jnp.int32),
            pltpu.VMEM((1, rays), jnp.int32),
            pltpu.VMEM((3, rays), F32),
            pltpu.VMEM((CELLS, 2 * WIDE), BF16),
            pltpu.VMEM((3, DEPTH, ROWS, WIDE), F32),
            pltpu.VMEM((DEPTH, ROWS, WIDE), F32),
            pltpu.VMEM((DEPTH, ROWS, WIDE), F32),
            pltpu.VMEM(block, F32),
            pltpu.VMEM((CELLS, WIDE), F32),
            pltpu.VMEM((slabs, WIDE, group), BF16),
            pltpu.VMEM((slabs, KEYS, group), BF16),
            pltpu.VMEM((2, 8, ROWS, WIDE), F32),
            pltpu.VMEM((24, ROWS, WIDE), F32),
            pltpu.VMEM((slabs, 4, group), F32),
            pltpu.VMEM((slabs, 4, group), F32),
            pltpu.VMEM((slabs, 4, group), F32),
            pltpu.VMEM((slabs, 4, group), F32),
            pltpu.VMEM((2, 1, 128), F32),
            pltpu.VMEM((n_a, 1, 128), F32),
            pltpu.VMEM((n_b, 1, 128), F32),
            dma,
            dma((4,)),
            dma((2,)),
            dma((2,)),
            dma((2,)),
            dma,
            dma((slabs,)),
            dma((2,)),
            dma((2,)),
            pltpu.SemaphoreType.REGULAR,
        ],
        compiler_params=pltpu.CompilerParams(collective_id=0, has_side_effects=True),
        name="render_gradient",
    )(
        voxel_grid,
        first_moment,
        second_moment,
        pixel_index.reshape(1, rays),
        start_slab.reshape(1, rays),
        ray_count.reshape(1, rays),
        target,
    )
    limit = CLIP_RMS * math.sqrt(4.0 * total_depth * total_x * WIDE)
    return pl.pallas_call(
        functools.partial(update_kernel, limit),
        out_shape=[jax.ShapeDtypeStruct(block, F32)] * 3,
        in_specs=[inside] * 5,
        out_specs=[anywhere] * 3,
        scratch_shapes=[held, held, held, dma((3,))],
        compiler_params=pltpu.CompilerParams(vmem_limit_bytes=16 * 2**20),
        name="clipped_adam",
    )(grid, first, second, grad, total)


def solution(mesh):
    torus = Mesh(mesh.devices.reshape(mesh.shape["slab"], 4, 8, 2), AXES)
    cells = P(None, "slab", TILE, None)
    rays = P(TILE)
    return jax.shard_map(
        per_device,
        mesh=torus,
        in_specs=(cells, cells, cells, rays, rays, rays, P(None, TILE)),
        out_specs=(cells, cells, cells),
        check_vma=False,
    )
```

```python
import functools
import math

import jax
import jax.numpy as jnp
from jax import lax
from jax.experimental import pallas as pl
from jax.experimental.pallas import tpu as pltpu
from jax.sharding import Mesh
from jax.sharding import PartitionSpec as P

STEP = 20
AXES = ("slab", "tile_0", "tile_1", "tile_2")
TILE = AXES[1:]

RENDER_WEIGHT = 1000.0
TV_WEIGHT = 0.05
BACKGROUND = 1.0
STEP_SPAN = 4.0
CLIP_RMS = 0.25
LEARN_RATE = 0.02
BETA_ONE = 0.9
BETA_TWO = 0.99
EPSILON = 1e-08

MESH_ID = pl.DeviceIdType.MESH
F32 = jnp.float32
BF16 = jnp.bfloat16
DEPTH = 16
ROWS = 8
WIDE = 256
KEYS = DEPTH * ROWS
CELLS = 4 * KEYS


def split_bf16(value):
    high = value.astype(BF16)
    return high, (value - high.astype(F32)).astype(BF16)


def sigmoid(value):
    return 1.0 / (1.0 + jnp.exp(-value))


def gradient_kernel(
    sizes,
    step_width,
    grid_hbm,
    first_hbm,
    second_hbm,
    pixel_hbm,
    start_hbm,
    count_hbm,
    target_hbm,
    grid,
    first,
    second,
    grad,
    total_ref,
    pixel,
    start,
    count,
    target,
    table,
    shade,
    clear,
    share,
    smooth,
    spread,
    columns,
    chosens,
    rank,
    rank_half,
    edges,
    halo,
    out_part,
    in_part,
    out_cot,
    in_cot,
    mine,
    sums_a,
    sums_b,
    grid_sem,
    rays_sem,
    moment_sem,
    halo_sem,
    part_sem,
    cot_send,
    cot_recv,
    a_sem,
    b_sem,
    ready,
):
    slabs, size_x, size_y, cores = sizes
    group = pixel.shape[1] // slabs
    slab = lax.axis_index("slab")
    at_x = lax.axis_index("tile_0")
    at_y = lax.axis_index("tile_1")
    core = lax.axis_index("tile_2")
    tiles = size_x * size_y * cores
    tile = (at_x * size_y + at_y) * cores + core
    n_a = slabs * cores
    n_b = size_x * size_y
    lead = cores - 1
    leads = core == lead
    me_a = slab * cores + core
    me_b = at_x * size_y + at_y

    def remote(source, into, send, recv, device):
        return pltpu.make_async_remote_copy(
            src_ref=source,
            dst_ref=into,
            send_sem=send,
            recv_sem=recv,
            device_id=device,
            device_id_type=MESH_ID,
        )

    def signal(semaphore, device):
        pl.semaphore_signal(semaphore, inc=1, device_id=device, device_id_type=MESH_ID)

    def tile_device(index):
        return (slab, index // (size_y * cores), (index // cores) % size_y, index % cores)

    def far_first(size):
        return sorted(range(1, size), key=lambda off: -min(off, size - off))

    over_a = [(z, c) for z in far_first(slabs) + [0] for c in range(cores) if z or c]
    over_b = sorted(
        ((x, y) for x in range(size_x) for y in range(size_y) if x or y),
        key=lambda off: -min(off[0], size_x - off[0]) - min(off[1], size_y - off[1]),
    )

    def device_a(off):
        return ((slab + off[0]) % slabs, at_x, at_y, (core + off[1]) % cores)

    def device_b(off, at_core):
        return (slab, (at_x + off[0]) % size_x, (at_y + off[1]) % size_y, at_core)

    barrier = pltpu.get_barrier_semaphore()
    greet = [device_a(off) for off in over_a]
    greet += [device_b((0, y), core) for y in far_first(size_y)]
    greet += [device_b((x, 0), core) for x in far_first(size_x)]
    next_tile = tile_device((tile + 1) % tiles)
    prev_tile = tile_device((tile + tiles - 1) % tiles)
    greet += [next_tile, prev_tile]

    load_grid = pltpu.make_async_copy(grid_hbm, grid, grid_sem)
    load_grid.start()
    for device in greet:
        signal(barrier, device)
    ray_loads = [
        pltpu.make_async_copy(source, into, rays_sem.at[k])
        for k, (source, into) in enumerate(
            ((pixel_hbm, pixel), (start_hbm, start), (count_hbm, count), (target_hbm, target))
        )
    ]
    for load in ray_loads:
        load.start()
    moment_loads = [
        pltpu.make_async_copy(first_hbm, first, moment_sem.at[0]),
        pltpu.make_async_copy(second_hbm, second, moment_sem.at[1]),
    ]
    for load in moment_loads:
        load.start()

    row_at = lax.broadcasted_iota(jnp.int32, (ROWS, WIDE), 0)
    lane_at = lax.broadcasted_iota(jnp.int32, (ROWS, WIDE), 1)
    rank[...] = lax.broadcasted_iota(jnp.int32, (KEYS, 128), 0)
    rank_half[...] = lax.broadcasted_iota(jnp.int32, (WIDE, 128), 0).astype(F32).astype(BF16)
    spread[...] = jnp.zeros_like(spread)

    load_grid.wait()
    light = jnp.ones((ROWS, WIDE), F32)
    color = [jnp.zeros((ROWS, WIDE), F32) for _ in range(3)]
    pairs = []
    for z in range(DEPTH):
        raw = grid[0, z]
        soft = jnp.maximum(raw, 0.0) + jnp.log(1.0 + jnp.exp(-jnp.abs(raw)))
        stay = jnp.exp(-(soft * step_width))
        weight = light * (1.0 - stay)
        light = light * stay
        share[z] = weight
        clear[z] = light
        for c in range(3):
            tone = sigmoid(grid[c + 1, z])
            shade[c, z] = tone
            color[c] = color[c] + weight * tone
        pairs.append((*color, 1.0 - light))
        if z % 2:
            for c in range(4):
                high, low = split_bf16(jnp.concatenate([pairs[-2][c], pairs[-1][c]], axis=0))
                rows = pl.ds(c * KEYS + (z - 1) * ROWS, 2 * ROWS)
                table[rows, pl.ds(0, WIDE)] = high
                table[rows, pl.ds(WIDE, WIDE)] = low
    for load in ray_loads:
        load.wait()

    def partner(place):
        half = (place + 1) // 2
        return (slab + half * (2 * (place % 2) - 1) + slabs) % slabs

    def leader(other):
        return (other, at_x, at_y, lead)

    def packed_row(row):
        return jnp.broadcast_to(row.astype(F32), (16, group)).astype(BF16)

    def look_up(other):
        lanes = pl.ds(pl.multiple_of(other * group, group), group)
        cell = pixel[:, lanes]
        begin = start[:, lanes]
        taken = begin * DEPTH + count[:, lanes] - slab * DEPTH
        taken = jnp.where(begin <= slab, jnp.clip(taken, 0, DEPTH), 0)
        key = (taken - 1) * ROWS + lax.shift_right_logical(cell, 8)
        one = jnp.ones((16, 128), BF16)
        zero = jnp.zeros((16, 128), BF16)
        for ref, row, height in (
            (columns, packed_row(cell & (WIDE - 1)), WIDE),
            (chosens, packed_row(key), KEYS),
        ):
            for k in range(0, height, 16):
                level = rank_half[pl.ds(k, 16), :]
                for t in range(0, group, 128):
                    ref[other, pl.ds(k, 16), pl.ds(t, 128)] = jnp.where(
                        level == row[:, t : t + 128], one, zero
                    )
        rows = []
        for half in range(0, group, WIDE):
            column = columns[other, :, pl.ds(half, WIDE)]
            found = jnp.dot(
                table[...],
                jnp.concatenate([column, column], axis=0),
                preferred_element_type=F32,
            )
            for t in range(0, WIDE, 128):
                wanted = jnp.broadcast_to(key[:, half + t : half + t + 128], (ROWS, 128))
                kept = [jnp.zeros((ROWS, 128), F32) for _ in range(4)]
                for k in range(0, KEYS, ROWS):
                    hit = rank[pl.ds(k, ROWS), :] == wanted
                    for c in range(4):
                        piece = found[c * KEYS + k : c * KEYS + k + ROWS, t : t + 128]
                        kept[c] = jnp.where(hit, piece, kept[c])
                rows.append([jnp.sum(keep, axis=0, keepdims=True) for keep in kept])
        values = [jnp.concatenate([row[c] for row in rows], axis=1) for c in range(4)]
        values[3] = 1.0 - values[3]
        return jnp.concatenate(values, axis=0)

    def send_part(slot, into, other):
        remote(
            out_part.at[slot], in_part.at[into], part_sem.at[0], part_sem.at[1], leader(other)
        ).start()

    places = list(range(slabs - 1, 0, -1))
    early = places[: slabs // 2]
    for place in early:
        out_part[partner(place)] = look_up(partner(place))
    pl.semaphore_wait(barrier, len(greet))
    for place in early:
        send_part(partner(place), me_a, partner(place))
    for place in places[slabs // 2 :]:
        out_part[partner(place)] = look_up(partner(place))
        send_part(partner(place), me_a, partner(place))
    out_part[slab] = look_up(slab)
    goal = target[:, pl.ds(pl.multiple_of(slab * group, group), group)]

    @pl.when(jnp.logical_not(leads))
    def _():
        send_part(slab, me_a, slab)
        out_part[slabs] = jnp.concatenate([goal, jnp.zeros((1, group), F32)], axis=0)
        send_part(slabs, n_a, slab)

    for c in range(4):
        for z in range(DEPTH):
            k = c * DEPTH + z
            edges[0, k // ROWS, pl.ds(k % ROWS, 1), :] = grid[c, z, pl.ds(ROWS - 1, 1), :]
            edges[1, k // ROWS, pl.ds(k % ROWS, 1), :] = grid[c, z, pl.ds(0, 1), :]
    for source, into, device in (
        (edges.at[0], halo.at[pl.ds(8, 8)], next_tile),
        (edges.at[1], halo.at[pl.ds(16, 8)], prev_tile),
        (grid.at[:, DEPTH - 1], halo.at[pl.ds(0, 4)], device_a((1, 0))),
        (grid.at[:, 0], halo.at[pl.ds(4, 4)], device_a((slabs - 1, 0))),
    ):
        remote(source, into, halo_sem.at[0], halo_sem.at[1], device).start()

    def part_blocks(n):
        part = in_part.at[pl.ds(0, n)]
        return remote(part, part, part_sem.at[0], part_sem.at[1], next_tile)

    def cot_blocks(n, slot):
        cot = out_cot.at[pl.ds(0, n)]
        return remote(cot, cot, cot_send, cot_recv.at[slot], next_tile)

    @pl.when(leads)
    def _():
        for x in far_first(size_x):
            signal(ready.at[0], device_b((x, 0), lead))
        in_part[me_a] = out_part[slab]
        part_blocks(n_a).wait_recv()
        for c in range(cores):
            ahead = jnp.ones((1, group), F32)
            rendered = jnp.zeros((3, group), F32)
            reach = []
            for s in range(slabs):
                reach.append(ahead)
                part = in_part[s * cores + c]
                rendered = rendered + ahead * part[:3]
                ahead = ahead * part[3:]
            wish = goal if c == lead else in_part[n_a][:3]
            residual = RENDER_WEIGHT * (rendered + ahead * BACKGROUND - wish)
            beyond = jnp.full((3, group), BACKGROUND, F32)
            for s in range(slabs - 1, -1, -1):
                product = residual * beyond
                dark = product[0:1] + product[1:2] + product[2:3]
                out_cot[s * cores + c] = reach[s] * jnp.concatenate([residual, dark], axis=0)
                part = in_part[s * cores + c]
                beyond = part[:3] + part[3:] * beyond
        for place in places + [0]:
            other = partner(place)
            for c in range(cores):
                if place or c != lead:
                    remote(
                        out_cot.at[other * cores + c],
                        in_cot.at[slab],
                        cot_send,
                        cot_recv.at[slab],
                        (other, at_x, at_y, c),
                    ).start()
        in_cot[slab] = out_cot[slab * cores + lead]
        if size_x > 1:
            pl.semaphore_wait(ready.at[0], size_x - 1)
        for y in far_first(size_y):
            signal(ready.at[1], device_b((0, y), lead))

    def scatter(other, cot):
        high, low = split_bf16(cot)
        chosen = chosens[other]
        column = columns[other]
        left = jnp.concatenate(
            [
                jnp.concatenate([chosen * high[c : c + 1], chosen * low[c : c + 1]], axis=1)
                for c in range(4)
            ],
            axis=0,
        )
        return lax.dot_general(
            left,
            jnp.concatenate([column, column], axis=1),
            (((1,), (1,)), ((), ())),
            preferred_element_type=F32,
        )

    remote(halo, halo, halo_sem.at[0], halo_sem.at[1], next_tile).wait()

    def smooth_channel(c, carry):
        for z in range(DEPTH):
            value = grid[c, z]
            if z > 0:
                total = value - grid[c, z - 1]
            else:
                total = jnp.where(slab > 0, value - halo[c], 0.0)
            if z < DEPTH - 1:
                total += value - grid[c, z + 1]
            else:
                total += jnp.where(slab < slabs - 1, value - halo[4 + c], 0.0)
            line = (2 * c + z // ROWS, pl.ds(z % ROWS, 1), slice(None))
            below = jnp.where(
                row_at == 0, halo[8 + line[0], line[1], line[2]], pltpu.roll(value, 1, 0)
            )
            above = jnp.where(
                row_at == ROWS - 1,
                halo[16 + line[0], line[1], line[2]],
                pltpu.roll(value, ROWS - 1, 0),
            )
            total += jnp.where((row_at > 0) | (tile > 0), value - below, 0.0)
            total += jnp.where((row_at < ROWS - 1) | (tile < tiles - 1), value - above, 0.0)
            total += jnp.where(lane_at > 0, value - pltpu.roll(value, 1, 1), 0.0)
            total += jnp.where(lane_at < WIDE - 1, value - pltpu.roll(value, WIDE - 1, 1), 0.0)
            smooth[c, z] = (2.0 * TV_WEIGHT) * total
        return carry

    lax.fori_loop(0, 4, smooth_channel, 0)

    def scatter_arrived(place, carry):
        other = partner(place)

        @pl.when((place > 0) | jnp.logical_not(leads))
        def _():
            cot_blocks(1, other).wait_recv()

        spread[...] += scatter(other, in_cot[other])
        return carry

    lax.fori_loop(0, slabs, scatter_arrived, 0)

    later = [jnp.zeros((ROWS, WIDE), F32) for _ in range(3)]
    tail = jnp.zeros((ROWS, WIDE), F32)
    squares = jnp.zeros((ROWS, WIDE), F32)
    for z in range(DEPTH - 1, -1, -1):
        weight = share[z]
        light = clear[z]
        pull = jnp.zeros((ROWS, WIDE), F32)
        for c in range(3):
            tone = shade[c, z]
            later[c] = later[c] + spread[pl.ds(c * KEYS + z * ROWS, ROWS), :]
            pull = pull + tone * later[c]
            value = weight * later[c] * (tone * (1.0 - tone)) + smooth[c + 1, z]
            grad[c + 1, z] = value
            squares = squares + value * value
        tail = tail + spread[pl.ds(3 * KEYS + z * ROWS, ROWS), :] * light
        thick = pull * light - tail
        tail = tail + pull * weight
        value = thick * (step_width * sigmoid(grid[0, z])) + smooth[0, z]
        grad[0, z] = value
        squares = squares + value * value

    squares = squares[:, :128] + squares[:, 128:]
    own = jnp.sum(squares, axis=0, keepdims=True)
    mine[0] = own

    def send_a(other):
        remote(mine.at[0], sums_a.at[me_a], a_sem.at[0], a_sem.at[1], leader(other)).start()

    def blocks(sums, n, send, recv):
        some = sums.at[pl.ds(0, n)]
        return remote(some, some, send, recv, next_tile)

    for off in far_first(slabs):
        send_a((slab + off) % slabs)

    @pl.when(jnp.logical_not(leads))
    def _():
        send_a(slab)
        part_blocks(slabs + 1).wait_send()
        blocks(sums_a, slabs, a_sem.at[0], a_sem.at[1]).wait_send()
        for load in moment_loads:
            load.wait()
        blocks(sums_b, n_b, b_sem.at[0], b_sem.at[2]).wait_recv()

    @pl.when(leads)
    def _():
        sums_a[me_a] = own
        part_blocks(slabs - 1).wait_send()
        cot_blocks(n_a - 1, 0).wait_send()
        for load in moment_loads:
            load.wait()
        if size_y > 1:
            pl.semaphore_wait(ready.at[1], size_y - 1)
        blocks(sums_a, n_a - 1, a_sem.at[0], a_sem.at[1]).wait_recv()
        share_b = jnp.sum(sums_a[...], axis=0)
        mine[1] = share_b
        for off in over_b + [(0, 0)]:
            for c in range(cores):
                if off != (0, 0) or c != lead:
                    remote(
                        mine.at[1],
                        sums_b.at[me_b],
                        b_sem.at[1 if c == lead else 0],
                        b_sem.at[2],
                        device_b(off, c),
                    ).start()
        sums_b[me_b] = share_b
        blocks(sums_a, slabs - 1, a_sem.at[0], a_sem.at[1]).wait_send()
        blocks(sums_b, n_b, b_sem.at[0], b_sem.at[2]).wait_send()
        if n_b > 1:
            blocks(sums_b, n_b - 1, b_sem.at[1], b_sem.at[2]).wait()

    total_ref[...] = jnp.sum(sums_b[...], axis=0)


def update_kernel(limit, grid, first, second, grad, total, *rest):
    outs, held, sem = rest[:3], rest[3:6], rest[6]
    norm = jnp.sqrt(jnp.sum(total[...], axis=1, keepdims=True))
    scale = limit / jnp.maximum(norm, limit)
    for c in range(4):
        clipped = grad[c] * scale
        new_first = BETA_ONE * first[c] + (1.0 - BETA_ONE) * clipped
        new_second = BETA_TWO * second[c] + (1.0 - BETA_TWO) * clipped * clipped
        held[1][c] = new_first
        held[2][c] = new_second
        first_hat = new_first * (1.0 / (1.0 - BETA_ONE**STEP))
        second_hat = new_second * (1.0 / (1.0 - BETA_TWO**STEP))
        held[0][c] = grid[c] - LEARN_RATE * first_hat / (jnp.sqrt(second_hat) + EPSILON)
        for k in range(3):
            pltpu.make_async_copy(held[k].at[c], outs[k].at[c], sem.at[k]).start()
    for k in range(3):
        pltpu.make_async_copy(held[k], outs[k], sem.at[k]).wait()


def per_device(voxel_grid, first_moment, second_moment, pixel_index, start_slab, ray_count, target):
    sizes = tuple(lax.axis_size(axis) for axis in AXES)
    slabs = sizes[0]
    rays = pixel_index.shape[0]
    group = rays // slabs
    total_depth = DEPTH * slabs
    total_x = ROWS * math.prod(sizes[1:])
    n_a = slabs * sizes[3]
    n_b = sizes[1] * sizes[2]
    block = (4, DEPTH, ROWS, WIDE)
    dma = pltpu.SemaphoreType.DMA
    anywhere = pl.BlockSpec(memory_space=pl.ANY)
    inside = pl.BlockSpec(memory_space=pltpu.VMEM)
    held = pltpu.VMEM(block, F32)
    grid, first, second, grad, total = pl.pallas_call(
        functools.partial(gradient_kernel, sizes, STEP_SPAN / total_depth),
        out_shape=(held, held, held, held, pltpu.VMEM((1, 128), F32)),
        in_specs=[anywhere] * 7,
        out_specs=(inside,) * 5,
        scratch_shapes=[
            pltpu.VMEM((1, rays), jnp.int32),
            pltpu.VMEM((1, rays), jnp.int32),
            pltpu.VMEM((1, rays), jnp.int32),
            pltpu.VMEM((3, rays), F32),
            pltpu.VMEM((CELLS, 2 * WIDE), BF16),
            pltpu.VMEM((3, DEPTH, ROWS, WIDE), F32),
            pltpu.VMEM((DEPTH, ROWS, WIDE), F32),
            pltpu.VMEM((DEPTH, ROWS, WIDE), F32),
            pltpu.VMEM(block, F32),
            pltpu.VMEM((CELLS, WIDE), F32),
            pltpu.VMEM((slabs, WIDE, group), BF16),
            pltpu.VMEM((slabs, KEYS, group), BF16),
            pltpu.VMEM((KEYS, 128), jnp.int32),
            pltpu.VMEM((WIDE, 128), BF16),
            pltpu.VMEM((2, 8, ROWS, WIDE), F32),
            pltpu.VMEM((24, ROWS, WIDE), F32),
            pltpu.VMEM((slabs + 1, 4, group), F32),
            pltpu.VMEM((n_a + 1, 4, group), F32),
            pltpu.VMEM((n_a, 4, group), F32),
            pltpu.VMEM((slabs, 4, group), F32),
            pltpu.VMEM((2, 1, 128), F32),
            pltpu.VMEM((n_a, 1, 128), F32),
            pltpu.VMEM((n_b, 1, 128), F32),
            dma,
            dma((4,)),
            dma((2,)),
            dma((2,)),
            dma((2,)),
            dma,
            dma((slabs,)),
            dma((2,)),
            dma((3,)),
            pltpu.SemaphoreType.REGULAR((2,)),
        ],
        compiler_params=pltpu.CompilerParams(collective_id=0, has_side_effects=True),
        name="render_gradient",
    )(
        voxel_grid,
        first_moment,
        second_moment,
        pixel_index.reshape(1, rays),
        start_slab.reshape(1, rays),
        ray_count.reshape(1, rays),
        target,
    )
    limit = CLIP_RMS * math.sqrt(4.0 * total_depth * total_x * WIDE)
    return pl.pallas_call(
        functools.partial(update_kernel, limit),
        out_shape=[jax.ShapeDtypeStruct(block, F32)] * 3,
        in_specs=[inside] * 5,
        out_specs=[anywhere] * 3,
        scratch_shapes=[held, held, held, dma((3,))],
        compiler_params=pltpu.CompilerParams(vmem_limit_bytes=16 * 2**20),
        name="clipped_adam",
    )(grid, first, second, grad, total)


def solution(mesh):
    torus = Mesh(mesh.devices.reshape(mesh.shape["slab"], 4, 8, 2), AXES)
    cells = P(None, "slab", TILE, None)
    rays = P(TILE)
    return jax.shard_map(
        per_device,
        mesh=torus,
        in_specs=(cells, cells, cells, rays, rays, rays, P(None, TILE)),
        out_specs=(cells, cells, cells),
        check_vma=False,
    )
```

```python
import functools
import math

import jax
import jax.numpy as jnp
from jax import lax
from jax.experimental import pallas as pl
from jax.experimental.pallas import tpu as pltpu
from jax.sharding import Mesh
from jax.sharding import PartitionSpec as P

STEP = 20
AXES = ("slab", "tile_0", "tile_1", "tile_2")
TILE = AXES[1:]

RENDER_WEIGHT = 1000.0
TV_WEIGHT = 0.05
BACKGROUND = 1.0
STEP_SPAN = 4.0
CLIP_RMS = 0.25
LEARN_RATE = 0.02
BETA_ONE = 0.9
BETA_TWO = 0.99
EPSILON = 1e-08

MESH_ID = pl.DeviceIdType.MESH
F32 = jnp.float32
BF16 = jnp.bfloat16
DEPTH = 16
ROWS = 8
WIDE = 256
KEYS = DEPTH * ROWS
CELLS = 4 * KEYS


def split_bf16(value):
    high = value.astype(BF16)
    return high, (value - high.astype(F32)).astype(BF16)


def sigmoid(value):
    return 1.0 / (1.0 + jnp.exp(-value))


def gradient_kernel(
    sizes,
    step_width,
    grid_hbm,
    first_hbm,
    second_hbm,
    pixel_hbm,
    start_hbm,
    count_hbm,
    target_hbm,
    grid,
    first,
    second,
    grad,
    total_ref,
    pixel,
    start,
    count,
    target,
    table,
    shade,
    clear,
    share,
    smooth,
    spread,
    columns,
    upright,
    chosens,
    rank,
    rank_half,
    edges,
    halo,
    out_part,
    in_part,
    out_cot,
    in_cot,
    mine,
    sums_a,
    sums_b,
    grid_sem,
    rays_sem,
    moment_sem,
    halo_sem,
    part_sem,
    cot_send,
    cot_recv,
    a_sem,
    b_sem,
    ready,
):
    slabs, size_x, size_y, cores = sizes
    group = pixel.shape[1] // slabs
    slab = lax.axis_index("slab")
    at_x = lax.axis_index("tile_0")
    at_y = lax.axis_index("tile_1")
    core = lax.axis_index("tile_2")
    tiles = size_x * size_y * cores
    tile = (at_x * size_y + at_y) * cores + core
    n_a = slabs * cores
    n_b = size_x * size_y
    lead = cores - 1
    leads = core == lead
    me_a = slab * cores + core
    me_b = at_x * size_y + at_y

    def remote(source, into, send, recv, device):
        return pltpu.make_async_remote_copy(
            src_ref=source,
            dst_ref=into,
            send_sem=send,
            recv_sem=recv,
            device_id=device,
            device_id_type=MESH_ID,
        )

    def signal(semaphore, device):
        pl.semaphore_signal(semaphore, inc=1, device_id=device, device_id_type=MESH_ID)

    def tile_device(index):
        return (slab, index // (size_y * cores), (index // cores) % size_y, index % cores)

    def far_first(size):
        return sorted(range(1, size), key=lambda off: -min(off, size - off))

    over_a = [(z, c) for z in far_first(slabs) + [0] for c in range(cores) if z or c]
    over_b = sorted(
        ((x, y) for x in range(size_x) for y in range(size_y) if x or y),
        key=lambda off: -min(off[0], size_x - off[0]) - min(off[1], size_y - off[1]),
    )

    def device_a(off):
        return ((slab + off[0]) % slabs, at_x, at_y, (core + off[1]) % cores)

    def device_b(off, at_core):
        return (slab, (at_x + off[0]) % size_x, (at_y + off[1]) % size_y, at_core)

    barrier = pltpu.get_barrier_semaphore()
    greet = [device_a(off) for off in over_a]
    greet += [device_b((0, y), core) for y in far_first(size_y)]
    greet += [device_b((x, 0), core) for x in far_first(size_x)]
    next_tile = tile_device((tile + 1) % tiles)
    prev_tile = tile_device((tile + tiles - 1) % tiles)
    greet += [next_tile, prev_tile]

    load_grid = pltpu.make_async_copy(grid_hbm, grid, grid_sem)
    load_grid.start()
    for device in greet:
        signal(barrier, device)
    ray_loads = [
        pltpu.make_async_copy(source, into, rays_sem.at[k])
        for k, (source, into) in enumerate(
            ((pixel_hbm, pixel), (start_hbm, start), (count_hbm, count), (target_hbm, target))
        )
    ]
    for load in ray_loads:
        load.start()
    moment_loads = [
        pltpu.make_async_copy(first_hbm, first, moment_sem.at[0]),
        pltpu.make_async_copy(second_hbm, second, moment_sem.at[1]),
    ]
    for load in moment_loads:
        load.start()

    row_at = lax.broadcasted_iota(jnp.int32, (ROWS, WIDE), 0)
    lane_at = lax.broadcasted_iota(jnp.int32, (ROWS, WIDE), 1)
    rank[...] = lax.broadcasted_iota(jnp.int32, (KEYS, 128), 0)
    rank_half[...] = lax.broadcasted_iota(jnp.int32, (WIDE, 128), 0).astype(F32).astype(BF16)
    spread[...] = jnp.zeros_like(spread)

    load_grid.wait()
    light = jnp.ones((ROWS, WIDE), F32)
    color = [jnp.zeros((ROWS, WIDE), F32) for _ in range(3)]
    pairs = []
    for z in range(DEPTH):
        raw = grid[0, z]
        soft = jnp.maximum(raw, 0.0) + jnp.log(1.0 + jnp.exp(-jnp.abs(raw)))
        stay = jnp.exp(-(soft * step_width))
        weight = light * (1.0 - stay)
        light = light * stay
        share[z] = weight
        clear[z] = light
        for c in range(3):
            tone = sigmoid(grid[c + 1, z])
            shade[c, z] = tone
            color[c] = color[c] + weight * tone
        pairs.append((*color, 1.0 - light))
        if z % 2:
            for c in range(4):
                high, low = split_bf16(jnp.concatenate([pairs[-2][c], pairs[-1][c]], axis=0))
                at = c * KEYS + (z - 1) * ROWS
                table[pl.ds(at, 2 * ROWS), :] = high
                table[pl.ds(CELLS + at, 2 * ROWS), :] = low
    for load in ray_loads:
        load.wait()

    def partner(place):
        half = (place + 1) // 2
        return (slab + half * (2 * (place % 2) - 1) + slabs) % slabs

    def leader(other):
        return (other, at_x, at_y, lead)

    def packed_row(row):
        return jnp.broadcast_to(row.astype(F32), (16, group)).astype(BF16)

    def look_up(other):
        lanes = pl.ds(pl.multiple_of(other * group, group), group)
        cell = pixel[:, lanes]
        begin = start[:, lanes]
        taken = begin * DEPTH + count[:, lanes] - slab * DEPTH
        taken = jnp.where(begin <= slab, jnp.clip(taken, 0, DEPTH), 0)
        key = (taken - 1) * ROWS + lax.shift_right_logical(cell, 8)
        one = jnp.ones((16, 128), BF16)
        zero = jnp.zeros((16, 128), BF16)
        for ref, row, height in (
            (columns, packed_row(cell & (WIDE - 1)), WIDE),
            (chosens, packed_row(key), KEYS),
        ):
            for k in range(0, height, 16):
                level = rank_half[pl.ds(k, 16), :]
                for t in range(0, group, 128):
                    ref[other, pl.ds(k, 16), pl.ds(t, 128)] = jnp.where(
                        level == row[:, t : t + 128], one, zero
                    )
        rows = []
        for half in range(0, group, WIDE):
            found = jnp.dot(
                table[...], columns[other, :, pl.ds(half, WIDE)], preferred_element_type=F32
            )
            for t in range(0, WIDE, 128):
                wanted = jnp.broadcast_to(key[:, half + t : half + t + 128], (ROWS, 128))
                kept = [jnp.zeros((ROWS, 128), F32) for _ in range(4)]
                for k in range(0, KEYS, ROWS):
                    hit = rank[pl.ds(k, ROWS), :] == wanted
                    for c in range(4):
                        high, low = (
                            found[at + c * KEYS + k : at + c * KEYS + k + ROWS, t : t + 128]
                            for at in (0, CELLS)
                        )
                        kept[c] = jnp.where(hit, high + low, kept[c])
                rows.append([jnp.sum(keep, axis=0, keepdims=True) for keep in kept])
        values = [jnp.concatenate([row[c] for row in rows], axis=1) for c in range(4)]
        values[3] = 1.0 - values[3]
        return jnp.concatenate(values, axis=0)

    def send_part(slot, into, other):
        remote(
            out_part.at[slot], in_part.at[into], part_sem.at[0], part_sem.at[1], leader(other)
        ).start()

    places = list(range(slabs - 1, 0, -1))
    early = places[: slabs // 2]
    for place in early:
        out_part[partner(place)] = look_up(partner(place))
    pl.semaphore_wait(barrier, len(greet))
    for place in early:
        send_part(partner(place), me_a, partner(place))
    for place in places[slabs // 2 :]:
        out_part[partner(place)] = look_up(partner(place))
        send_part(partner(place), me_a, partner(place))
    out_part[slab] = look_up(slab)
    goal = target[:, pl.ds(pl.multiple_of(slab * group, group), group)]

    @pl.when(jnp.logical_not(leads))
    def _():
        send_part(slab, me_a, slab)
        out_part[slabs] = jnp.concatenate([goal, jnp.zeros((1, group), F32)], axis=0)
        send_part(slabs, n_a, slab)

    for c in range(4):
        for z in range(DEPTH):
            k = c * DEPTH + z
            edges[0, k // ROWS, pl.ds(k % ROWS, 1), :] = grid[c, z, pl.ds(ROWS - 1, 1), :]
            edges[1, k // ROWS, pl.ds(k % ROWS, 1), :] = grid[c, z, pl.ds(0, 1), :]
    for source, into, device in (
        (edges.at[0], halo.at[pl.ds(8, 8)], next_tile),
        (edges.at[1], halo.at[pl.ds(16, 8)], prev_tile),
        (grid.at[:, DEPTH - 1], halo.at[pl.ds(0, 4)], device_a((1, 0))),
        (grid.at[:, 0], halo.at[pl.ds(4, 4)], device_a((slabs - 1, 0))),
    ):
        remote(source, into, halo_sem.at[0], halo_sem.at[1], device).start()

    def stand_up(other, carry):
        cell = pixel[:, pl.ds(pl.multiple_of(other * group, group), group)]
        column = (cell & (WIDE - 1)).astype(F32)
        level = lax.broadcasted_iota(jnp.int32, (16, WIDE), 1).astype(F32).astype(BF16)
        one = jnp.ones((16, WIDE), BF16)
        zero = jnp.zeros((16, WIDE), BF16)
        for t in range(0, group, 128):
            down = jnp.broadcast_to(column[:, t : t + 128], (128, 128)).T.astype(BF16)
            for k in range(0, 128, 16):
                tall = down[k : k + 16]
                upright[other, pl.ds(t + k, 16), :] = jnp.where(
                    jnp.concatenate([tall] * (WIDE // 128), axis=1) == level, one, zero
                )
        return carry

    lax.fori_loop(0, slabs, stand_up, 0)

    def part_blocks(n):
        part = in_part.at[pl.ds(0, n)]
        return remote(part, part, part_sem.at[0], part_sem.at[1], next_tile)

    def cot_blocks(n, slot):
        cot = out_cot.at[pl.ds(0, n)]
        return remote(cot, cot, cot_send, cot_recv.at[slot], next_tile)

    @pl.when(leads)
    def _():
        for x in far_first(size_x):
            signal(ready.at[0], device_b((x, 0), lead))
        in_part[me_a] = out_part[slab]
        part_blocks(n_a).wait_recv()
        for c in range(cores):
            ahead = jnp.ones((1, group), F32)
            rendered = jnp.zeros((3, group), F32)
            reach = []
            for s in range(slabs):
                reach.append(ahead)
                part = in_part[s * cores + c]
                rendered = rendered + ahead * part[:3]
                ahead = ahead * part[3:]
            wish = goal if c == lead else in_part[n_a][:3]
            residual = RENDER_WEIGHT * (rendered + ahead * BACKGROUND - wish)
            beyond = jnp.full((3, group), BACKGROUND, F32)
            for s in range(slabs - 1, -1, -1):
                product = residual * beyond
                dark = product[0:1] + product[1:2] + product[2:3]
                out_cot[s * cores + c] = reach[s] * jnp.concatenate([residual, dark], axis=0)
                part = in_part[s * cores + c]
                beyond = part[:3] + part[3:] * beyond
        for place in range(slabs):
            other = partner(place)
            for c in range(cores):
                if place or c != lead:
                    remote(
                        out_cot.at[other * cores + c],
                        in_cot.at[slab],
                        cot_send,
                        cot_recv.at[slab],
                        (other, at_x, at_y, c),
                    ).start()
        in_cot[slab] = out_cot[slab * cores + lead]
        if size_x > 1:
            pl.semaphore_wait(ready.at[0], size_x - 1)
        for y in far_first(size_y):
            signal(ready.at[1], device_b((0, y), lead))

    def scatter(other, cot):
        high, low = split_bf16(cot)
        chosen = chosens[other]
        left = jnp.concatenate(
            [chosen * half[c : c + 1] for half in (high, low) for c in range(4)], axis=0
        )
        found = jnp.dot(left, upright[other], preferred_element_type=F32)
        return found[:CELLS] + found[CELLS:]

    remote(halo, halo, halo_sem.at[0], halo_sem.at[1], next_tile).wait()

    def smooth_channel(c, carry):
        for z in range(DEPTH):
            value = grid[c, z]
            if z > 0:
                total = value - grid[c, z - 1]
            else:
                total = jnp.where(slab > 0, value - halo[c], 0.0)
            if z < DEPTH - 1:
                total += value - grid[c, z + 1]
            else:
                total += jnp.where(slab < slabs - 1, value - halo[4 + c], 0.0)
            line = (2 * c + z // ROWS, pl.ds(z % ROWS, 1), slice(None))
            below = jnp.where(
                row_at == 0, halo[8 + line[0], line[1], line[2]], pltpu.roll(value, 1, 0)
            )
            above = jnp.where(
                row_at == ROWS - 1,
                halo[16 + line[0], line[1], line[2]],
                pltpu.roll(value, ROWS - 1, 0),
            )
            total += jnp.where((row_at > 0) | (tile > 0), value - below, 0.0)
            total += jnp.where((row_at < ROWS - 1) | (tile < tiles - 1), value - above, 0.0)
            total += jnp.where(lane_at > 0, value - pltpu.roll(value, 1, 1), 0.0)
            total += jnp.where(lane_at < WIDE - 1, value - pltpu.roll(value, WIDE - 1, 1), 0.0)
            smooth[c, z] = (2.0 * TV_WEIGHT) * total
        return carry

    lax.fori_loop(0, 4, smooth_channel, 0)

    def scatter_arrived(place, carry):
        other = partner(place)

        @pl.when((place > 0) | jnp.logical_not(leads))
        def _():
            cot_blocks(1, other).wait_recv()

        spread[...] += scatter(other, in_cot[other])
        return carry

    lax.fori_loop(0, slabs, scatter_arrived, 0)

    later = [jnp.zeros((ROWS, WIDE), F32) for _ in range(3)]
    tail = jnp.zeros((ROWS, WIDE), F32)
    squares = jnp.zeros((ROWS, WIDE), F32)
    for z in range(DEPTH - 1, -1, -1):
        weight = share[z]
        light = clear[z]
        pull = jnp.zeros((ROWS, WIDE), F32)
        for c in range(3):
            tone = shade[c, z]
            later[c] = later[c] + spread[pl.ds(c * KEYS + z * ROWS, ROWS), :]
            pull = pull + tone * later[c]
            value = weight * later[c] * (tone * (1.0 - tone)) + smooth[c + 1, z]
            grad[c + 1, z] = value
            squares = squares + value * value
        tail = tail + spread[pl.ds(3 * KEYS + z * ROWS, ROWS), :] * light
        thick = pull * light - tail
        tail = tail + pull * weight
        value = thick * (step_width * sigmoid(grid[0, z])) + smooth[0, z]
        grad[0, z] = value
        squares = squares + value * value

    squares = squares[:, :128] + squares[:, 128:]
    own = jnp.sum(squares, axis=0, keepdims=True)
    mine[0] = own

    def send_a(other):
        remote(mine.at[0], sums_a.at[me_a], a_sem.at[0], a_sem.at[1], leader(other)).start()

    def blocks(sums, n, send, recv):
        some = sums.at[pl.ds(0, n)]
        return remote(some, some, send, recv, next_tile)

    for off in far_first(slabs):
        send_a((slab + off) % slabs)

    @pl.when(jnp.logical_not(leads))
    def _():
        send_a(slab)
        part_blocks(slabs + 1).wait_send()
        blocks(sums_a, slabs, a_sem.at[0], a_sem.at[1]).wait_send()
        for load in moment_loads:
            load.wait()
        blocks(sums_b, n_b, b_sem.at[0], b_sem.at[2]).wait_recv()

    @pl.when(leads)
    def _():
        sums_a[me_a] = own
        part_blocks(slabs - 1).wait_send()
        cot_blocks(n_a - 1, 0).wait_send()
        for load in moment_loads:
            load.wait()
        if size_y > 1:
            pl.semaphore_wait(ready.at[1], size_y - 1)
        blocks(sums_a, n_a - 1, a_sem.at[0], a_sem.at[1]).wait_recv()
        share_b = jnp.sum(sums_a[...], axis=0)
        mine[1] = share_b
        for off in over_b + [(0, 0)]:
            for c in range(cores):
                if off != (0, 0) or c != lead:
                    remote(
                        mine.at[1],
                        sums_b.at[me_b],
                        b_sem.at[1 if c == lead else 0],
                        b_sem.at[2],
                        device_b(off, c),
                    ).start()
        sums_b[me_b] = share_b
        blocks(sums_a, slabs - 1, a_sem.at[0], a_sem.at[1]).wait_send()
        blocks(sums_b, n_b, b_sem.at[0], b_sem.at[2]).wait_send()
        if n_b > 1:
            blocks(sums_b, n_b - 1, b_sem.at[1], b_sem.at[2]).wait()

    total_ref[...] = jnp.sum(sums_b[...], axis=0)


def update_kernel(limit, grid, first, second, grad, total, *rest):
    outs, held, sem = rest[:3], rest[3:6], rest[6]
    norm = jnp.sqrt(jnp.sum(total[...], axis=1, keepdims=True))
    scale = limit / jnp.maximum(norm, limit)
    for c in range(4):
        clipped = grad[c] * scale
        new_first = BETA_ONE * first[c] + (1.0 - BETA_ONE) * clipped
        new_second = BETA_TWO * second[c] + (1.0 - BETA_TWO) * clipped * clipped
        held[1][c] = new_first
        held[2][c] = new_second
        first_hat = new_first * (1.0 / (1.0 - BETA_ONE**STEP))
        second_hat = new_second * (1.0 / (1.0 - BETA_TWO**STEP))
        held[0][c] = grid[c] - LEARN_RATE * first_hat / (jnp.sqrt(second_hat) + EPSILON)
        for k in range(3):
            pltpu.make_async_copy(held[k].at[c], outs[k].at[c], sem.at[k]).start()
    for k in range(3):
        pltpu.make_async_copy(held[k], outs[k], sem.at[k]).wait()


def per_device(voxel_grid, first_moment, second_moment, pixel_index, start_slab, ray_count, target):
    sizes = tuple(lax.axis_size(axis) for axis in AXES)
    slabs = sizes[0]
    rays = pixel_index.shape[0]
    group = rays // slabs
    total_depth = DEPTH * slabs
    total_x = ROWS * math.prod(sizes[1:])
    n_a = slabs * sizes[3]
    n_b = sizes[1] * sizes[2]
    block = (4, DEPTH, ROWS, WIDE)
    dma = pltpu.SemaphoreType.DMA
    anywhere = pl.BlockSpec(memory_space=pl.ANY)
    inside = pl.BlockSpec(memory_space=pltpu.VMEM)
    held = pltpu.VMEM(block, F32)
    grid, first, second, grad, total = pl.pallas_call(
        functools.partial(gradient_kernel, sizes, STEP_SPAN / total_depth),
        out_shape=(held, held, held, held, pltpu.VMEM((1, 128), F32)),
        in_specs=[anywhere] * 7,
        out_specs=(inside,) * 5,
        scratch_shapes=[
            pltpu.VMEM((1, rays), jnp.int32),
            pltpu.VMEM((1, rays), jnp.int32),
            pltpu.VMEM((1, rays), jnp.int32),
            pltpu.VMEM((3, rays), F32),
            pltpu.VMEM((2 * CELLS, WIDE), BF16),
            pltpu.VMEM((3, DEPTH, ROWS, WIDE), F32),
            pltpu.VMEM((DEPTH, ROWS, WIDE), F32),
            pltpu.VMEM((DEPTH, ROWS, WIDE), F32),
            pltpu.VMEM(block, F32),
            pltpu.VMEM((CELLS, WIDE), F32),
            pltpu.VMEM((slabs, WIDE, group), BF16),
            pltpu.VMEM((slabs, group, WIDE), BF16),
            pltpu.VMEM((slabs, KEYS, group), BF16),
            pltpu.VMEM((KEYS, 128), jnp.int32),
            pltpu.VMEM((WIDE, 128), BF16),
            pltpu.VMEM((2, 8, ROWS, WIDE), F32),
            pltpu.VMEM((24, ROWS, WIDE), F32),
            pltpu.VMEM((slabs + 1, 4, group), F32),
            pltpu.VMEM((n_a + 1, 4, group), F32),
            pltpu.VMEM((n_a, 4, group), F32),
            pltpu.VMEM((slabs, 4, group), F32),
            pltpu.VMEM((2, 1, 128), F32),
            pltpu.VMEM((n_a, 1, 128), F32),
            pltpu.VMEM((n_b, 1, 128), F32),
            dma,
            dma((4,)),
            dma((2,)),
            dma((2,)),
            dma((2,)),
            dma,
            dma((slabs,)),
            dma((2,)),
            dma((3,)),
            pltpu.SemaphoreType.REGULAR((2,)),
        ],
        compiler_params=pltpu.CompilerParams(collective_id=0, has_side_effects=True),
        name="render_gradient",
    )(
        voxel_grid,
        first_moment,
        second_moment,
        pixel_index.reshape(1, rays),
        start_slab.reshape(1, rays),
        ray_count.reshape(1, rays),
        target,
    )
    limit = CLIP_RMS * math.sqrt(4.0 * total_depth * total_x * WIDE)
    return pl.pallas_call(
        functools.partial(update_kernel, limit),
        out_shape=[jax.ShapeDtypeStruct(block, F32)] * 3,
        in_specs=[inside] * 5,
        out_specs=[anywhere] * 3,
        scratch_shapes=[held, held, held, dma((3,))],
        compiler_params=pltpu.CompilerParams(vmem_limit_bytes=16 * 2**20),
        name="clipped_adam",
    )(grid, first, second, grad, total)


def solution(mesh):
    torus = Mesh(mesh.devices.reshape(mesh.shape["slab"], 4, 8, 2), AXES)
    cells = P(None, "slab", TILE, None)
    rays = P(TILE)
    return jax.shard_map(
        per_device,
        mesh=torus,
        in_specs=(cells, cells, cells, rays, rays, rays, P(None, TILE)),
        out_specs=(cells, cells, cells),
        check_vma=False,
    )
```

```python
import functools
import math

import jax
import jax.numpy as jnp
from jax import lax
from jax.experimental import pallas as pl
from jax.experimental.pallas import tpu as pltpu
from jax.sharding import Mesh
from jax.sharding import PartitionSpec as P

STEP = 20
AXES = ("slab", "tile_0", "tile_1", "tile_2")
TILE = AXES[1:]

RENDER_WEIGHT = 1000.0
TV_WEIGHT = 0.05
BACKGROUND = 1.0
STEP_SPAN = 4.0
CLIP_RMS = 0.25
LEARN_RATE = 0.02
BETA_ONE = 0.9
BETA_TWO = 0.99
EPSILON = 1e-08

MESH_ID = pl.DeviceIdType.MESH
F32 = jnp.float32
BF16 = jnp.bfloat16
DEPTH = 16
ROWS = 8
WIDE = 256
KEYS = DEPTH * ROWS
CELLS = 4 * KEYS


def split_bf16(value):
    high = value.astype(BF16)
    return high, (value - high.astype(F32)).astype(BF16)


def sigmoid(value):
    return 1.0 / (1.0 + jnp.exp(-value))


def gradient_kernel(
    sizes,
    step_width,
    grid_hbm,
    first_hbm,
    second_hbm,
    pixel_hbm,
    start_hbm,
    count_hbm,
    target_hbm,
    grid,
    first,
    second,
    grad,
    total_ref,
    pixel,
    start,
    count,
    target,
    table,
    shade,
    clear,
    share,
    smooth,
    spread,
    columns,
    upright,
    chosens,
    rank,
    rank_half,
    edges,
    halo,
    out_part,
    in_part,
    out_cot,
    in_cot,
    mine,
    sums_a,
    sums_b,
    grid_sem,
    rays_sem,
    moment_sem,
    halo_sem,
    part_sem,
    cot_send,
    cot_recv,
    a_sem,
    b_sem,
    ready,
):
    slabs, size_x, size_y, cores = sizes
    group = pixel.shape[1] // slabs
    slab = lax.axis_index("slab")
    at_x = lax.axis_index("tile_0")
    at_y = lax.axis_index("tile_1")
    core = lax.axis_index("tile_2")
    tiles = size_x * size_y * cores
    tile = (at_x * size_y + at_y) * cores + core
    n_a = slabs * cores
    n_b = size_x * size_y
    lead = cores - 1
    leads = core == lead
    me_a = slab * cores + core
    me_b = at_x * size_y + at_y

    def remote(source, into, send, recv, device):
        return pltpu.make_async_remote_copy(
            src_ref=source,
            dst_ref=into,
            send_sem=send,
            recv_sem=recv,
            device_id=device,
            device_id_type=MESH_ID,
        )

    def signal(semaphore, device):
        pl.semaphore_signal(semaphore, inc=1, device_id=device, device_id_type=MESH_ID)

    def tile_device(index):
        return (slab, index // (size_y * cores), (index // cores) % size_y, index % cores)

    def far_first(size):
        return sorted(range(1, size), key=lambda off: -min(off, size - off))

    over_a = [(z, c) for z in far_first(slabs) + [0] for c in range(cores) if z or c]
    over_b = sorted(
        ((x, y) for x in range(size_x) for y in range(size_y) if x or y),
        key=lambda off: -min(off[0], size_x - off[0]) - min(off[1], size_y - off[1]),
    )

    def device_a(off):
        return ((slab + off[0]) % slabs, at_x, at_y, (core + off[1]) % cores)

    def device_b(off, at_core):
        return (slab, (at_x + off[0]) % size_x, (at_y + off[1]) % size_y, at_core)

    barrier = pltpu.get_barrier_semaphore()
    greet = [device_a(off) for off in over_a]
    assert size_y <= 8
    two_away = [y for y in far_first(size_y) if min(y, size_y - y) == 2] if size_y > 4 else []
    greet += [
        device_b((0, y), c)
        for y in far_first(size_y)
        if min(y, size_y - y) <= 2
        for c in range(cores)
    ]
    greet += [device_b((x, 0), core) for x in far_first(size_x)]
    next_tile = tile_device((tile + 1) % tiles)
    prev_tile = tile_device((tile + tiles - 1) % tiles)
    greet += [next_tile, prev_tile]

    load_grid = pltpu.make_async_copy(grid_hbm, grid, grid_sem)
    load_grid.start()
    for device in greet:
        signal(barrier, device)
    ray_loads = [
        pltpu.make_async_copy(source, into, rays_sem.at[k])
        for k, (source, into) in enumerate(
            ((pixel_hbm, pixel), (start_hbm, start), (count_hbm, count), (target_hbm, target))
        )
    ]
    for load in ray_loads:
        load.start()
    moment_loads = [
        pltpu.make_async_copy(first_hbm, first, moment_sem.at[0]),
        pltpu.make_async_copy(second_hbm, second, moment_sem.at[1]),
    ]

    row_at = lax.broadcasted_iota(jnp.int32, (ROWS, WIDE), 0)
    lane_at = lax.broadcasted_iota(jnp.int32, (ROWS, WIDE), 1)
    rank[...] = lax.broadcasted_iota(jnp.int32, (KEYS, 128), 0)
    rank_half[...] = lax.broadcasted_iota(jnp.int32, (WIDE, 128), 0).astype(F32).astype(BF16)

    load_grid.wait()
    for load in moment_loads:
        load.start()
    light = jnp.ones((ROWS, WIDE), F32)
    color = [jnp.zeros((ROWS, WIDE), F32) for _ in range(3)]
    pairs = []
    for z in range(DEPTH):
        raw = grid[0, z]
        soft = jnp.maximum(raw, 0.0) + jnp.log(1.0 + jnp.exp(-jnp.abs(raw)))
        stay = jnp.exp(-(soft * step_width))
        weight = light * (1.0 - stay)
        light = light * stay
        share[z] = weight
        clear[z] = light
        for c in range(3):
            tone = sigmoid(grid[c + 1, z])
            shade[c, z] = tone
            color[c] = color[c] + weight * tone
        pairs.append((*color, 1.0 - light))
        if z % 2:
            for c in range(4):
                high, low = split_bf16(jnp.concatenate([pairs[-2][c], pairs[-1][c]], axis=0))
                at = c * KEYS + (z - 1) * ROWS
                table[pl.ds(at, 2 * ROWS), :] = high
                table[pl.ds(CELLS + at, 2 * ROWS), :] = low
    for load in ray_loads:
        load.wait()

    def partner(place):
        half = (place + 1) // 2
        return (slab + half * (2 * (place % 2) - 1) + slabs) % slabs

    def leader(other):
        return (other, at_x, at_y, lead)

    def packed_row(row):
        return jnp.broadcast_to(row.astype(F32), (16, group)).astype(BF16)

    def look_up(other):
        lanes = pl.ds(pl.multiple_of(other * group, group), group)
        cell = pixel[:, lanes]
        begin = start[:, lanes]
        taken = begin * DEPTH + count[:, lanes] - slab * DEPTH
        taken = jnp.where(begin <= slab, jnp.clip(taken, 0, DEPTH), 0)
        key = (taken - 1) * ROWS + lax.shift_right_logical(cell, 8)
        one = jnp.ones((16, 128), BF16)
        zero = jnp.zeros((16, 128), BF16)
        for ref, row, height in (
            (columns, packed_row(cell & (WIDE - 1)), WIDE),
            (chosens, packed_row(key), KEYS),
        ):
            for k in range(0, height, 16):
                level = rank_half[pl.ds(k, 16), :]
                for t in range(0, group, 128):
                    ref[other, pl.ds(k, 16), pl.ds(t, 128)] = jnp.where(
                        level == row[:, t : t + 128], one, zero
                    )
        rows = []
        for half in range(0, group, WIDE):
            found = jnp.dot(
                table[...], columns[other, :, pl.ds(half, WIDE)], preferred_element_type=F32
            )
            for t in range(0, WIDE, 128):
                wanted = jnp.broadcast_to(key[:, half + t : half + t + 128], (ROWS, 128))
                kept = [jnp.zeros((ROWS, 128), F32) for _ in range(4)]
                for k in range(0, KEYS, ROWS):
                    hit = rank[pl.ds(k, ROWS), :] == wanted
                    for c in range(4):
                        high, low = (
                            found[at + c * KEYS + k : at + c * KEYS + k + ROWS, t : t + 128]
                            for at in (0, CELLS)
                        )
                        kept[c] = jnp.where(hit, high + low, kept[c])
                rows.append([jnp.sum(keep, axis=0, keepdims=True) for keep in kept])
        values = [jnp.concatenate([row[c] for row in rows], axis=1) for c in range(4)]
        values[3] = 1.0 - values[3]
        return jnp.concatenate(values, axis=0)

    def send_part(slot, into, other):
        remote(
            out_part.at[slot], in_part.at[into], part_sem.at[0], part_sem.at[1], leader(other)
        ).start()

    places = list(range(slabs - 1, 0, -1))
    early = places[: slabs // 2]
    for place in early:
        out_part[partner(place)] = look_up(partner(place))
    pl.semaphore_wait(barrier, len(greet))
    for place in early:
        send_part(partner(place), me_a, partner(place))
    for place in places[slabs // 2 :]:
        out_part[partner(place)] = look_up(partner(place))
        send_part(partner(place), me_a, partner(place))
    out_part[slab] = look_up(slab)
    goal = target[:, pl.ds(pl.multiple_of(slab * group, group), group)]

    @pl.when(jnp.logical_not(leads))
    def _():
        send_part(slab, me_a, slab)
        out_part[slabs] = jnp.concatenate([goal, jnp.zeros((1, group), F32)], axis=0)
        send_part(slabs, n_a, slab)

    for c in range(4):
        for z in range(DEPTH):
            k = c * DEPTH + z
            edges[0, k // ROWS, pl.ds(k % ROWS, 1), :] = grid[c, z, pl.ds(ROWS - 1, 1), :]
            edges[1, k // ROWS, pl.ds(k % ROWS, 1), :] = grid[c, z, pl.ds(0, 1), :]
    for source, into, device in (
        (edges.at[0], halo.at[pl.ds(8, 8)], next_tile),
        (edges.at[1], halo.at[pl.ds(16, 8)], prev_tile),
        (grid.at[:, DEPTH - 1], halo.at[pl.ds(0, 4)], device_a((1, 0))),
        (grid.at[:, 0], halo.at[pl.ds(4, 4)], device_a((slabs - 1, 0))),
    ):
        remote(source, into, halo_sem.at[0], halo_sem.at[1], device).start()

    def stand_up(other, carry):
        cell = pixel[:, pl.ds(pl.multiple_of(other * group, group), group)]
        column = (cell & (WIDE - 1)).astype(F32)
        level = lax.broadcasted_iota(jnp.int32, (16, WIDE), 1).astype(F32).astype(BF16)
        one = jnp.ones((16, WIDE), BF16)
        zero = jnp.zeros((16, WIDE), BF16)
        for t in range(0, group, 128):
            down = jnp.broadcast_to(column[:, t : t + 128], (128, 128)).T.astype(BF16)
            for k in range(0, 128, 16):
                tall = down[k : k + 16]
                upright[other, pl.ds(t + k, 16), :] = jnp.where(
                    jnp.concatenate([tall] * (WIDE // 128), axis=1) == level, one, zero
                )
        return carry

    lax.fori_loop(0, slabs, stand_up, 0)

    def part_blocks(n):
        part = in_part.at[pl.ds(0, n)]
        return remote(part, part, part_sem.at[0], part_sem.at[1], next_tile)

    def cot_blocks(n, slot):
        cot = out_cot.at[pl.ds(0, n)]
        return remote(cot, cot, cot_send, cot_recv.at[slot], next_tile)

    @pl.when(leads)
    def _():
        for y in two_away:
            signal(ready.at[0], device_b((0, y), lead))
        in_part[me_a] = out_part[slab]
        part_blocks(n_a).wait_recv()
        for c in range(cores):
            ahead = jnp.ones((1, group), F32)
            rendered = jnp.zeros((3, group), F32)
            reach = []
            for s in range(slabs):
                reach.append(ahead)
                part = in_part[s * cores + c]
                rendered = rendered + ahead * part[:3]
                ahead = ahead * part[3:]
            wish = goal if c == lead else in_part[n_a][:3]
            residual = RENDER_WEIGHT * (rendered + ahead * BACKGROUND - wish)
            beyond = jnp.full((3, group), BACKGROUND, F32)
            for s in range(slabs - 1, -1, -1):
                product = residual * beyond
                dark = product[0:1] + product[1:2] + product[2:3]
                out_cot[s * cores + c] = reach[s] * jnp.concatenate([residual, dark], axis=0)
                part = in_part[s * cores + c]
                beyond = part[:3] + part[3:] * beyond
        for place in range(slabs):
            other = partner(place)
            for c in range(cores):
                if place or c != lead:
                    remote(
                        out_cot.at[other * cores + c],
                        in_cot.at[slab],
                        cot_send,
                        cot_recv.at[slab],
                        (other, at_x, at_y, c),
                    ).start()
        in_cot[slab] = out_cot[slab * cores + lead]
        if two_away:
            pl.semaphore_wait(ready.at[0], len(two_away))
        for x in far_first(size_x):
            signal(ready.at[1], device_b((x, 0), lead))

    def scatter(others):
        right = jnp.concatenate([upright[other] for other in others], axis=0)
        halves = [split_bf16(in_cot[other]) for other in others]
        found = [
            jnp.dot(
                jnp.concatenate(
                    [
                        jnp.concatenate(
                            [chosens[other] * half[part][c : c + 1] for c in range(4)], axis=0
                        )
                        for other, half in zip(others, halves)
                    ],
                    axis=1,
                ),
                right,
                preferred_element_type=F32,
            )
            for part in (0, 1)
        ]
        return found[0] + found[1]

    remote(halo, halo, halo_sem.at[0], halo_sem.at[1], next_tile).wait()

    def smooth_channel(c, carry):
        for z in range(DEPTH):
            value = grid[c, z]
            if z > 0:
                total = value - grid[c, z - 1]
            else:
                total = jnp.where(slab > 0, value - halo[c], 0.0)
            if z < DEPTH - 1:
                total += value - grid[c, z + 1]
            else:
                total += jnp.where(slab < slabs - 1, value - halo[4 + c], 0.0)
            line = (2 * c + z // ROWS, pl.ds(z % ROWS, 1), slice(None))
            below = jnp.where(
                row_at == 0, halo[8 + line[0], line[1], line[2]], pltpu.roll(value, 1, 0)
            )
            above = jnp.where(
                row_at == ROWS - 1,
                halo[16 + line[0], line[1], line[2]],
                pltpu.roll(value, ROWS - 1, 0),
            )
            total += jnp.where((row_at > 0) | (tile > 0), value - below, 0.0)
            total += jnp.where((row_at < ROWS - 1) | (tile < tiles - 1), value - above, 0.0)
            total += jnp.where(lane_at > 0, value - pltpu.roll(value, 1, 1), 0.0)
            total += jnp.where(lane_at < WIDE - 1, value - pltpu.roll(value, WIDE - 1, 1), 0.0)
            smooth[c, z] = (2.0 * TV_WEIGHT) * total
        return carry

    lax.fori_loop(0, 4, smooth_channel, 0)

    @pl.when(jnp.logical_not(leads))
    def _():
        cot_blocks(1, slab).wait_recv()

    spread[...] = scatter([slab])
    for first_place, past in ((1, 3), (3, 5), (5, 8)):
        arrived = [partner(place) for place in range(first_place, min(past, slabs))]
        for other in arrived:
            cot_blocks(1, other).wait_recv()
        if arrived:
            spread[...] += scatter(arrived)

    later = [jnp.zeros((ROWS, WIDE), F32) for _ in range(3)]
    tail = jnp.zeros((ROWS, WIDE), F32)
    squares = jnp.zeros((ROWS, WIDE), F32)
    for z in range(DEPTH - 1, -1, -1):
        weight = share[z]
        light = clear[z]
        pull = jnp.zeros((ROWS, WIDE), F32)
        for c in range(3):
            tone = shade[c, z]
            later[c] = later[c] + spread[pl.ds(c * KEYS + z * ROWS, ROWS), :]
            pull = pull + tone * later[c]
            value = weight * later[c] * (tone * (1.0 - tone)) + smooth[c + 1, z]
            grad[c + 1, z] = value
            squares = squares + value * value
        tail = tail + spread[pl.ds(3 * KEYS + z * ROWS, ROWS), :] * light
        thick = pull * light - tail
        tail = tail + pull * weight
        value = thick * (step_width * sigmoid(grid[0, z])) + smooth[0, z]
        grad[0, z] = value
        squares = squares + value * value

    squares = squares[:, :128] + squares[:, 128:]
    own = jnp.sum(squares, axis=0, keepdims=True)
    mine[0] = own

    def send_a(other):
        remote(mine.at[0], sums_a.at[me_a], a_sem.at[0], a_sem.at[1], leader(other)).start()

    def blocks(sums, n, send, recv):
        some = sums.at[pl.ds(0, n)]
        return remote(some, some, send, recv, next_tile)

    for off in far_first(slabs):
        send_a((slab + off) % slabs)

    @pl.when(jnp.logical_not(leads))
    def _():
        send_a(slab)
        part_blocks(slabs + 1).wait_send()
        blocks(sums_a, slabs, a_sem.at[0], a_sem.at[1]).wait_send()
        for load in moment_loads:
            load.wait()
        blocks(sums_b, n_b, b_sem.at[0], b_sem.at[2]).wait_recv()

    @pl.when(leads)
    def _():
        sums_a[me_a] = own
        part_blocks(slabs - 1).wait_send()
        cot_blocks(n_a - 1, 0).wait_send()
        for load in moment_loads:
            load.wait()
        if size_x > 1:
            pl.semaphore_wait(ready.at[1], size_x - 1)
        blocks(sums_a, n_a - 1, a_sem.at[0], a_sem.at[1]).wait_recv()
        share_b = jnp.sum(sums_a[...], axis=0)
        mine[1] = share_b
        for off in over_b + [(0, 0)]:
            for c in range(cores):
                if off != (0, 0) or c != lead:
                    remote(
                        mine.at[1],
                        sums_b.at[me_b],
                        b_sem.at[1 if c == lead else 0],
                        b_sem.at[2],
                        device_b(off, c),
                    ).start()
        sums_b[me_b] = share_b
        blocks(sums_a, slabs - 1, a_sem.at[0], a_sem.at[1]).wait_send()
        blocks(sums_b, n_b, b_sem.at[0], b_sem.at[2]).wait_send()
        if n_b > 1:
            blocks(sums_b, n_b - 1, b_sem.at[1], b_sem.at[2]).wait()

    total_ref[...] = jnp.sum(sums_b[...], axis=0)


def update_kernel(limit, grid, first, second, grad, total, *rest):
    outs, held, sem = rest[:3], rest[3:6], rest[6]
    norm = jnp.sqrt(jnp.sum(total[...], axis=1, keepdims=True))
    scale = jnp.broadcast_to(limit / jnp.maximum(norm, limit), (ROWS, WIDE))
    rate = LEARN_RATE / (1.0 - BETA_ONE**STEP)
    for c in range(4):
        for z in range(DEPTH):
            clipped = grad[c, z] * scale
            new_first = BETA_ONE * first[c, z] + (1.0 - BETA_ONE) * clipped
            new_second = BETA_TWO * second[c, z] + ((1.0 - BETA_TWO) * clipped) * clipped
            second_hat = new_second * (1.0 / (1.0 - BETA_TWO**STEP))
            root = second_hat * lax.rsqrt(second_hat)
            held[0][c, z] = grid[c, z] - (rate * new_first) * pl.reciprocal(root + EPSILON)
            held[1][c, z] = new_first
            held[2][c, z] = new_second
        for k in range(3):
            pltpu.make_async_copy(held[k].at[c], outs[k].at[c], sem.at[k]).start()
    for k in range(3):
        pltpu.make_async_copy(held[k], outs[k], sem.at[k]).wait()


def per_device(voxel_grid, first_moment, second_moment, pixel_index, start_slab, ray_count, target):
    sizes = tuple(lax.axis_size(axis) for axis in AXES)
    slabs = sizes[0]
    rays = pixel_index.shape[0]
    group = rays // slabs
    total_depth = DEPTH * slabs
    total_x = ROWS * math.prod(sizes[1:])
    n_a = slabs * sizes[3]
    n_b = sizes[1] * sizes[2]
    block = (4, DEPTH, ROWS, WIDE)
    dma = pltpu.SemaphoreType.DMA
    anywhere = pl.BlockSpec(memory_space=pl.ANY)
    inside = pl.BlockSpec(memory_space=pltpu.VMEM)
    held = pltpu.VMEM(block, F32)
    grid, first, second, grad, total = pl.pallas_call(
        functools.partial(gradient_kernel, sizes, STEP_SPAN / total_depth),
        out_shape=(held, held, held, held, pltpu.VMEM((1, 128), F32)),
        in_specs=[anywhere] * 7,
        out_specs=(inside,) * 5,
        scratch_shapes=[
            pltpu.VMEM((1, rays), jnp.int32),
            pltpu.VMEM((1, rays), jnp.int32),
            pltpu.VMEM((1, rays), jnp.int32),
            pltpu.VMEM((3, rays), F32),
            pltpu.VMEM((2 * CELLS, WIDE), BF16),
            pltpu.VMEM((3, DEPTH, ROWS, WIDE), F32),
            pltpu.VMEM((DEPTH, ROWS, WIDE), F32),
            pltpu.VMEM((DEPTH, ROWS, WIDE), F32),
            pltpu.VMEM(block, F32),
            pltpu.VMEM((CELLS, WIDE), F32),
            pltpu.VMEM((slabs, WIDE, group), BF16),
            pltpu.VMEM((slabs, group, WIDE), BF16),
            pltpu.VMEM((slabs, KEYS, group), BF16),
            pltpu.VMEM((KEYS, 128), jnp.int32),
            pltpu.VMEM((WIDE, 128), BF16),
            pltpu.VMEM((2, 8, ROWS, WIDE), F32),
            pltpu.VMEM((24, ROWS, WIDE), F32),
            pltpu.VMEM((slabs + 1, 4, group), F32),
            pltpu.VMEM((n_a + 1, 4, group), F32),
            pltpu.VMEM((n_a, 4, group), F32),
            pltpu.VMEM((slabs, 4, group), F32),
            pltpu.VMEM((2, 1, 128), F32),
            pltpu.VMEM((n_a, 1, 128), F32),
            pltpu.VMEM((n_b, 1, 128), F32),
            dma,
            dma((4,)),
            dma((2,)),
            dma((2,)),
            dma((2,)),
            dma,
            dma((slabs,)),
            dma((2,)),
            dma((3,)),
            pltpu.SemaphoreType.REGULAR((2,)),
        ],
        compiler_params=pltpu.CompilerParams(collective_id=0, has_side_effects=True),
        name="render_gradient",
    )(
        voxel_grid,
        first_moment,
        second_moment,
        pixel_index.reshape(1, rays),
        start_slab.reshape(1, rays),
        ray_count.reshape(1, rays),
        target,
    )
    limit = CLIP_RMS * math.sqrt(4.0 * total_depth * total_x * WIDE)
    return pl.pallas_call(
        functools.partial(update_kernel, limit),
        out_shape=[jax.ShapeDtypeStruct(block, F32)] * 3,
        in_specs=[inside] * 5,
        out_specs=[anywhere] * 3,
        scratch_shapes=[held, held, held, dma((3,))],
        compiler_params=pltpu.CompilerParams(vmem_limit_bytes=16 * 2**20),
        name="clipped_adam",
    )(grid, first, second, grad, total)


def solution(mesh):
    torus = Mesh(mesh.devices.reshape(mesh.shape["slab"], 4, 8, 2), AXES)
    cells = P(None, "slab", TILE, None)
    rays = P(TILE)
    return jax.shard_map(
        per_device,
        mesh=torus,
        in_specs=(cells, cells, cells, rays, rays, rays, P(None, TILE)),
        out_specs=(cells, cells, cells),
        check_vma=False,
    )
```

```python
import functools
import math

import jax
import jax.numpy as jnp
from jax import lax
from jax.experimental import pallas as pl
from jax.experimental.pallas import tpu as pltpu
from jax.sharding import Mesh
from jax.sharding import PartitionSpec as P

STEP = 20
AXES = ("slab", "tile_0", "tile_1", "tile_2")
TILE = AXES[1:]

RENDER_WEIGHT = 1000.0
TV_WEIGHT = 0.05
BACKGROUND = 1.0
STEP_SPAN = 4.0
CLIP_RMS = 0.25
LEARN_RATE = 0.02
BETA_ONE = 0.9
BETA_TWO = 0.99
EPSILON = 1e-08

MESH_ID = pl.DeviceIdType.MESH
F32 = jnp.float32
BF16 = jnp.bfloat16
DEPTH = 16
ROWS = 8
WIDE = 256
KEYS = DEPTH * ROWS
CELLS = 4 * KEYS


def split_bf16(value):
    high = value.astype(BF16)
    return high, (value - high.astype(F32)).astype(BF16)


def sigmoid(value):
    return 1.0 / (1.0 + jnp.exp(-value))


def gradient_kernel(
    sizes,
    step_width,
    grid_hbm,
    first_hbm,
    second_hbm,
    pixel_hbm,
    start_hbm,
    count_hbm,
    target_hbm,
    grid,
    first,
    second,
    grad,
    total_ref,
    pixel,
    start,
    count,
    target,
    table,
    shade,
    clear,
    share,
    smooth,
    spread,
    columns,
    upright,
    chosens,
    rank,
    rank_half,
    edges,
    halo,
    out_part,
    in_part,
    out_cot,
    in_cot,
    mine,
    sums_a,
    sums_b,
    grid_sem,
    rays_sem,
    moment_sem,
    halo_sem,
    part_sem,
    cot_send,
    cot_recv,
    a_sem,
    b_sem,
    ready,
):
    slabs, size_x, size_y, cores = sizes
    group = pixel.shape[1] // slabs
    slab = lax.axis_index("slab")
    at_x = lax.axis_index("tile_0")
    at_y = lax.axis_index("tile_1")
    core = lax.axis_index("tile_2")
    tiles = size_x * size_y * cores
    tile = (at_x * size_y + at_y) * cores + core
    n_a = slabs * cores
    n_b = size_x * size_y
    lead = cores - 1
    leads = core == lead
    me_a = slab * cores + core
    me_b = at_x * size_y + at_y

    def remote(source, into, send, recv, device):
        return pltpu.make_async_remote_copy(
            src_ref=source,
            dst_ref=into,
            send_sem=send,
            recv_sem=recv,
            device_id=device,
            device_id_type=MESH_ID,
        )

    def signal(semaphore, device):
        pl.semaphore_signal(semaphore, inc=1, device_id=device, device_id_type=MESH_ID)

    def tile_device(index):
        return (slab, index // (size_y * cores), (index // cores) % size_y, index % cores)

    def far_first(size):
        return sorted(range(1, size), key=lambda off: -min(off, size - off))

    over_a = [(z, c) for z in far_first(slabs) + [0] for c in range(cores) if z or c]
    over_b = sorted(
        ((x, y) for x in range(size_x) for y in range(size_y) if x or y),
        key=lambda off: -min(off[0], size_x - off[0]) - min(off[1], size_y - off[1]),
    )

    def device_a(off):
        return ((slab + off[0]) % slabs, at_x, at_y, (core + off[1]) % cores)

    def device_b(off, at_core):
        return (slab, (at_x + off[0]) % size_x, (at_y + off[1]) % size_y, at_core)

    barrier = pltpu.get_barrier_semaphore()
    greet = [device_a(off) for off in over_a]
    assert size_y <= 8
    two_away = [y for y in far_first(size_y) if min(y, size_y - y) == 2] if size_y > 4 else []
    greet += [
        device_b((0, y), c)
        for y in far_first(size_y)
        if min(y, size_y - y) <= 2
        for c in range(cores)
    ]
    greet += [device_b((x, 0), core) for x in far_first(size_x)]
    next_tile = tile_device((tile + 1) % tiles)
    prev_tile = tile_device((tile + tiles - 1) % tiles)
    greet += [next_tile, prev_tile]

    load_grid = pltpu.make_async_copy(grid_hbm, grid, grid_sem)
    load_grid.start()
    for device in greet:
        signal(barrier, device)
    ray_loads = [
        pltpu.make_async_copy(source, into, rays_sem.at[k])
        for k, (source, into) in enumerate(
            ((pixel_hbm, pixel), (start_hbm, start), (count_hbm, count), (target_hbm, target))
        )
    ]
    for load in ray_loads:
        load.start()
    moment_loads = [
        pltpu.make_async_copy(first_hbm, first, moment_sem.at[0]),
        pltpu.make_async_copy(second_hbm, second, moment_sem.at[1]),
    ]

    row_at = lax.broadcasted_iota(jnp.int32, (ROWS, WIDE), 0)
    lane_at = lax.broadcasted_iota(jnp.int32, (ROWS, WIDE), 1)
    rank[...] = lax.broadcasted_iota(jnp.int32, (KEYS, 128), 0)
    rank_half[...] = lax.broadcasted_iota(jnp.int32, (WIDE, 128), 0).astype(F32).astype(BF16)

    spread[...] = jnp.zeros_like(spread)

    load_grid.wait()
    for load in moment_loads:
        load.start()
    light = jnp.ones((ROWS, WIDE), F32)
    color = [jnp.zeros((ROWS, WIDE), F32) for _ in range(3)]
    pairs = []
    for z in range(DEPTH):
        raw = grid[0, z]
        soft = jnp.maximum(raw, 0.0) + jnp.log(1.0 + jnp.exp(-jnp.abs(raw)))
        stay = jnp.exp(-(soft * step_width))
        weight = light * (1.0 - stay)
        light = light * stay
        share[z] = weight
        clear[z] = light
        for c in range(3):
            tone = sigmoid(grid[c + 1, z])
            shade[c, z] = tone
            color[c] = color[c] + weight * tone
        pairs.append((*color, 1.0 - light))
        if z % 2:
            for c in range(4):
                high, low = split_bf16(jnp.concatenate([pairs[-2][c], pairs[-1][c]], axis=0))
                at = c * KEYS + (z - 1) * ROWS
                table[pl.ds(at, 2 * ROWS), :] = high
                table[pl.ds(CELLS + at, 2 * ROWS), :] = low
    for load in ray_loads:
        load.wait()

    def partner(place):
        half = (place + 1) // 2
        return (slab + half * (2 * (place % 2) - 1) + slabs) % slabs

    def leader(other):
        return (other, at_x, at_y, lead)

    def packed_row(row):
        return jnp.broadcast_to(row.astype(F32), (16, group)).astype(BF16)

    def look_up(other):
        lanes = pl.ds(pl.multiple_of(other * group, group), group)
        cell = pixel[:, lanes]
        begin = start[:, lanes]
        taken = begin * DEPTH + count[:, lanes] - slab * DEPTH
        taken = jnp.where(begin <= slab, jnp.clip(taken, 0, DEPTH), 0)
        key = (taken - 1) * ROWS + lax.shift_right_logical(cell, 8)
        one = jnp.ones((16, 128), BF16)
        zero = jnp.zeros((16, 128), BF16)
        for ref, row, height in (
            (columns, packed_row(cell & (WIDE - 1)), WIDE),
            (chosens, packed_row(key), KEYS),
        ):
            for k in range(0, height, 16):
                level = rank_half[pl.ds(k, 16), :]
                for t in range(0, group, 128):
                    ref[other, pl.ds(k, 16), pl.ds(t, 128)] = jnp.where(
                        level == row[:, t : t + 128], one, zero
                    )
        rows = []
        for half in range(0, group, WIDE):
            found = jnp.dot(
                table[...], columns[other, :, pl.ds(half, WIDE)], preferred_element_type=F32
            )
            for t in range(0, WIDE, 128):
                wanted = jnp.broadcast_to(key[:, half + t : half + t + 128], (ROWS, 128))
                kept = [jnp.zeros((ROWS, 128), F32) for _ in range(4)]
                for k in range(0, KEYS, ROWS):
                    hit = rank[pl.ds(k, ROWS), :] == wanted
                    for c in range(4):
                        high, low = (
                            found[at + c * KEYS + k : at + c * KEYS + k + ROWS, t : t + 128]
                            for at in (0, CELLS)
                        )
                        kept[c] = jnp.where(hit, high + low, kept[c])
                rows.append([jnp.sum(keep, axis=0, keepdims=True) for keep in kept])
        values = [jnp.concatenate([row[c] for row in rows], axis=1) for c in range(4)]
        values[3] = 1.0 - values[3]
        return jnp.concatenate(values, axis=0)

    def send_part(slot, into, other):
        remote(
            out_part.at[slot], in_part.at[into], part_sem.at[0], part_sem.at[1], leader(other)
        ).start()

    places = list(range(slabs - 1, 0, -1))
    early = places[: slabs // 2]
    for place in early:
        out_part[partner(place)] = look_up(partner(place))
    pl.semaphore_wait(barrier, len(greet))
    for place in early:
        send_part(partner(place), me_a, partner(place))

    @pl.when(leads)
    def _():
        for y in two_away:
            signal(ready.at[0], device_b((0, y), lead))

    for place in places[slabs // 2 :]:
        out_part[partner(place)] = look_up(partner(place))
        send_part(partner(place), me_a, partner(place))
    out_part[slab] = look_up(slab)
    goal = target[:, pl.ds(pl.multiple_of(slab * group, group), group)]

    @pl.when(jnp.logical_not(leads))
    def _():
        send_part(slab, me_a, slab)
        out_part[slabs] = jnp.concatenate([goal, jnp.zeros((1, group), F32)], axis=0)
        send_part(slabs, n_a, slab)

    for c in range(4):
        for z in range(DEPTH):
            k = c * DEPTH + z
            edges[0, k // ROWS, pl.ds(k % ROWS, 1), :] = grid[c, z, pl.ds(ROWS - 1, 1), :]
            edges[1, k // ROWS, pl.ds(k % ROWS, 1), :] = grid[c, z, pl.ds(0, 1), :]
    for source, into, device in (
        (edges.at[0], halo.at[pl.ds(8, 8)], next_tile),
        (edges.at[1], halo.at[pl.ds(16, 8)], prev_tile),
        (grid.at[:, DEPTH - 1], halo.at[pl.ds(0, 4)], device_a((1, 0))),
        (grid.at[:, 0], halo.at[pl.ds(4, 4)], device_a((slabs - 1, 0))),
    ):
        remote(source, into, halo_sem.at[0], halo_sem.at[1], device).start()

    def stand_up(other, carry):
        cell = pixel[:, pl.ds(pl.multiple_of(other * group, group), group)]
        column = (cell & (WIDE - 1)).astype(F32)
        level = lax.broadcasted_iota(jnp.int32, (16, WIDE), 1).astype(F32).astype(BF16)
        one = jnp.ones((16, WIDE), BF16)
        zero = jnp.zeros((16, WIDE), BF16)
        for t in range(0, group, 128):
            down = jnp.broadcast_to(column[:, t : t + 128], (128, 128)).T.astype(BF16)
            for k in range(0, 128, 16):
                tall = down[k : k + 16]
                upright[other, pl.ds(t + k, 16), :] = jnp.where(
                    jnp.concatenate([tall] * (WIDE // 128), axis=1) == level, one, zero
                )
        return carry

    lax.fori_loop(0, slabs, stand_up, 0)

    def part_blocks(n):
        part = in_part.at[pl.ds(0, n)]
        return remote(part, part, part_sem.at[0], part_sem.at[1], next_tile)

    def cot_blocks(n, slot):
        cot = out_cot.at[pl.ds(0, n)]
        return remote(cot, cot, cot_send, cot_recv.at[slot], next_tile)

    @pl.when(leads)
    def _():
        in_part[me_a] = out_part[slab]
        part_blocks(n_a).wait_recv()
        for c in range(cores):
            ahead = jnp.ones((1, group), F32)
            rendered = jnp.zeros((3, group), F32)
            reach = []
            for s in range(slabs):
                reach.append(ahead)
                part = in_part[s * cores + c]
                rendered = rendered + ahead * part[:3]
                ahead = ahead * part[3:]
            wish = goal if c == lead else in_part[n_a][:3]
            residual = RENDER_WEIGHT * (rendered + ahead * BACKGROUND - wish)
            beyond = jnp.full((3, group), BACKGROUND, F32)
            for s in range(slabs - 1, -1, -1):
                product = residual * beyond
                dark = product[0:1] + product[1:2] + product[2:3]
                out_cot[s * cores + c] = reach[s] * jnp.concatenate([residual, dark], axis=0)
                part = in_part[s * cores + c]
                beyond = part[:3] + part[3:] * beyond
        for place in range(slabs):
            other = partner(place)
            for c in range(cores):
                if place or c != lead:
                    remote(
                        out_cot.at[other * cores + c],
                        in_cot.at[slab],
                        cot_send,
                        cot_recv.at[slab],
                        (other, at_x, at_y, c),
                    ).start()
        in_cot[slab] = out_cot[slab * cores + lead]

    def scatter(other):
        high, low = split_bf16(in_cot[other])
        chosen = chosens[other]
        left = jnp.concatenate(
            [chosen * half[c : c + 1] for half in (high, low) for c in range(4)], axis=0
        )
        found = jnp.dot(left, upright[other], preferred_element_type=F32)
        return found[:CELLS] + found[CELLS:]

    remote(halo, halo, halo_sem.at[0], halo_sem.at[1], next_tile).wait()

    def smooth_channel(c, carry):
        for z in range(DEPTH):
            value = grid[c, z]
            if z > 0:
                total = value - grid[c, z - 1]
            else:
                total = jnp.where(slab > 0, value - halo[c], 0.0)
            if z < DEPTH - 1:
                total += value - grid[c, z + 1]
            else:
                total += jnp.where(slab < slabs - 1, value - halo[4 + c], 0.0)
            line = (2 * c + z // ROWS, pl.ds(z % ROWS, 1), slice(None))
            below = jnp.where(
                row_at == 0, halo[8 + line[0], line[1], line[2]], pltpu.roll(value, 1, 0)
            )
            above = jnp.where(
                row_at == ROWS - 1,
                halo[16 + line[0], line[1], line[2]],
                pltpu.roll(value, ROWS - 1, 0),
            )
            total += jnp.where((row_at > 0) | (tile > 0), value - below, 0.0)
            total += jnp.where((row_at < ROWS - 1) | (tile < tiles - 1), value - above, 0.0)
            total += jnp.where(lane_at > 0, value - pltpu.roll(value, 1, 1), 0.0)
            total += jnp.where(lane_at < WIDE - 1, value - pltpu.roll(value, WIDE - 1, 1), 0.0)
            smooth[c, z] = (2.0 * TV_WEIGHT) * total
        return carry

    lax.fori_loop(0, 4, smooth_channel, 0)

    @pl.when(leads)
    def _():
        if two_away:
            pl.semaphore_wait(ready.at[0], len(two_away))
        for x in far_first(size_x):
            signal(ready.at[1], device_b((x, 0), lead))


    def scatter_arrived(place, carry):
        other = partner(place)

        @pl.when((place > 0) | jnp.logical_not(leads))
        def _():
            cot_blocks(1, other).wait_recv()

        spread[...] += scatter(other)
        return carry

    lax.fori_loop(0, slabs, scatter_arrived, 0)

    later = [jnp.zeros((ROWS, WIDE), F32) for _ in range(3)]
    tail = jnp.zeros((ROWS, WIDE), F32)
    squares = jnp.zeros((ROWS, WIDE), F32)
    for z in range(DEPTH - 1, -1, -1):
        weight = share[z]
        light = clear[z]
        pull = jnp.zeros((ROWS, WIDE), F32)
        for c in range(3):
            tone = shade[c, z]
            later[c] = later[c] + spread[pl.ds(c * KEYS + z * ROWS, ROWS), :]
            pull = pull + tone * later[c]
            value = weight * later[c] * (tone * (1.0 - tone)) + smooth[c + 1, z]
            grad[c + 1, z] = value
            squares = squares + value * value
        tail = tail + spread[pl.ds(3 * KEYS + z * ROWS, ROWS), :] * light
        thick = pull * light - tail
        tail = tail + pull * weight
        value = thick * (step_width * sigmoid(grid[0, z])) + smooth[0, z]
        grad[0, z] = value
        squares = squares + value * value

    squares = squares[:, :128] + squares[:, 128:]
    own = jnp.sum(squares, axis=0, keepdims=True)
    mine[0] = own

    def send_a(other):
        remote(mine.at[0], sums_a.at[me_a], a_sem.at[0], a_sem.at[1], leader(other)).start()

    def blocks(sums, n, send, recv):
        some = sums.at[pl.ds(0, n)]
        return remote(some, some, send, recv, next_tile)

    for off in far_first(slabs):
        send_a((slab + off) % slabs)

    @pl.when(jnp.logical_not(leads))
    def _():
        send_a(slab)
        part_blocks(slabs + 1).wait_send()
        blocks(sums_a, slabs, a_sem.at[0], a_sem.at[1]).wait_send()
        for load in moment_loads:
            load.wait()
        blocks(sums_b, n_b, b_sem.at[0], b_sem.at[2]).wait_recv()

    @pl.when(leads)
    def _():
        sums_a[me_a] = own
        part_blocks(slabs - 1).wait_send()
        cot_blocks(n_a - 1, 0).wait_send()
        for load in moment_loads:
            load.wait()
        if size_x > 1:
            pl.semaphore_wait(ready.at[1], size_x - 1)
        blocks(sums_a, n_a - 1, a_sem.at[0], a_sem.at[1]).wait_recv()
        share_b = jnp.sum(sums_a[...], axis=0)
        mine[1] = share_b
        for off in over_b + [(0, 0)]:
            for c in range(cores):
                if off != (0, 0) or c != lead:
                    remote(
                        mine.at[1],
                        sums_b.at[me_b],
                        b_sem.at[1 if c == lead else 0],
                        b_sem.at[2],
                        device_b(off, c),
                    ).start()
        sums_b[me_b] = share_b
        blocks(sums_a, slabs - 1, a_sem.at[0], a_sem.at[1]).wait_send()
        blocks(sums_b, n_b, b_sem.at[0], b_sem.at[2]).wait_send()
        if n_b > 1:
            blocks(sums_b, n_b - 1, b_sem.at[1], b_sem.at[2]).wait()

    total_ref[...] = jnp.sum(sums_b[...], axis=0)


def update_kernel(limit, grid, first, second, grad, total, *rest):
    outs, held, sem = rest[:3], rest[3:6], rest[6]
    norm = jnp.sqrt(jnp.sum(total[...], axis=1, keepdims=True))
    scale = jnp.broadcast_to(limit / jnp.maximum(norm, limit), (ROWS, WIDE))
    rate = LEARN_RATE / (1.0 - BETA_ONE**STEP)
    for c in range(4):
        for z in range(DEPTH):
            clipped = grad[c, z] * scale
            new_first = BETA_ONE * first[c, z] + (1.0 - BETA_ONE) * clipped
            new_second = BETA_TWO * second[c, z] + ((1.0 - BETA_TWO) * clipped) * clipped
            second_hat = new_second * (1.0 / (1.0 - BETA_TWO**STEP))
            root = second_hat * lax.rsqrt(second_hat)
            held[0][c, z] = grid[c, z] - (rate * new_first) * pl.reciprocal(root + EPSILON)
            held[1][c, z] = new_first
            held[2][c, z] = new_second
        for k in range(3):
            pltpu.make_async_copy(held[k].at[c], outs[k].at[c], sem.at[k]).start()
    for k in range(3):
        pltpu.make_async_copy(held[k], outs[k], sem.at[k]).wait()


def per_device(voxel_grid, first_moment, second_moment, pixel_index, start_slab, ray_count, target):
    sizes = tuple(lax.axis_size(axis) for axis in AXES)
    slabs = sizes[0]
    rays = pixel_index.shape[0]
    group = rays // slabs
    total_depth = DEPTH * slabs
    total_x = ROWS * math.prod(sizes[1:])
    n_a = slabs * sizes[3]
    n_b = sizes[1] * sizes[2]
    block = (4, DEPTH, ROWS, WIDE)
    dma = pltpu.SemaphoreType.DMA
    anywhere = pl.BlockSpec(memory_space=pl.ANY)
    inside = pl.BlockSpec(memory_space=pltpu.VMEM)
    held = pltpu.VMEM(block, F32)
    grid, first, second, grad, total = pl.pallas_call(
        functools.partial(gradient_kernel, sizes, STEP_SPAN / total_depth),
        out_shape=(held, held, held, held, pltpu.VMEM((1, 128), F32)),
        in_specs=[anywhere] * 7,
        out_specs=(inside,) * 5,
        scratch_shapes=[
            pltpu.VMEM((1, rays), jnp.int32),
            pltpu.VMEM((1, rays), jnp.int32),
            pltpu.VMEM((1, rays), jnp.int32),
            pltpu.VMEM((3, rays), F32),
            pltpu.VMEM((2 * CELLS, WIDE), BF16),
            pltpu.VMEM((3, DEPTH, ROWS, WIDE), F32),
            pltpu.VMEM((DEPTH, ROWS, WIDE), F32),
            pltpu.VMEM((DEPTH, ROWS, WIDE), F32),
            pltpu.VMEM(block, F32),
            pltpu.VMEM((CELLS, WIDE), F32),
            pltpu.VMEM((slabs, WIDE, group), BF16),
            pltpu.VMEM((slabs, group, WIDE), BF16),
            pltpu.VMEM((slabs, KEYS, group), BF16),
            pltpu.VMEM((KEYS, 128), jnp.int32),
            pltpu.VMEM((WIDE, 128), BF16),
            pltpu.VMEM((2, 8, ROWS, WIDE), F32),
            pltpu.VMEM((24, ROWS, WIDE), F32),
            pltpu.VMEM((slabs + 1, 4, group), F32),
            pltpu.VMEM((n_a + 1, 4, group), F32),
            pltpu.VMEM((n_a, 4, group), F32),
            pltpu.VMEM((slabs, 4, group), F32),
            pltpu.VMEM((2, 1, 128), F32),
            pltpu.VMEM((n_a, 1, 128), F32),
            pltpu.VMEM((n_b, 1, 128), F32),
            dma,
            dma((4,)),
            dma((2,)),
            dma((2,)),
            dma((2,)),
            dma,
            dma((slabs,)),
            dma((2,)),
            dma((3,)),
            pltpu.SemaphoreType.REGULAR((2,)),
        ],
        compiler_params=pltpu.CompilerParams(collective_id=0, has_side_effects=True),
        name="render_gradient",
    )(
        voxel_grid,
        first_moment,
        second_moment,
        pixel_index.reshape(1, rays),
        start_slab.reshape(1, rays),
        ray_count.reshape(1, rays),
        target,
    )
    limit = CLIP_RMS * math.sqrt(4.0 * total_depth * total_x * WIDE)
    return pl.pallas_call(
        functools.partial(update_kernel, limit),
        out_shape=[jax.ShapeDtypeStruct(block, F32)] * 3,
        in_specs=[inside] * 5,
        out_specs=[anywhere] * 3,
        scratch_shapes=[held, held, held, dma((3,))],
        compiler_params=pltpu.CompilerParams(vmem_limit_bytes=16 * 2**20),
        name="clipped_adam",
    )(grid, first, second, grad, total)


def solution(mesh):
    torus = Mesh(mesh.devices.reshape(mesh.shape["slab"], 4, 8, 2), AXES)
    cells = P(None, "slab", TILE, None)
    rays = P(TILE)
    return jax.shard_map(
        per_device,
        mesh=torus,
        in_specs=(cells, cells, cells, rays, rays, rays, P(None, TILE)),
        out_specs=(cells, cells, cells),
        check_vma=False,
    )
```

```python
import functools
import math

import jax
import jax.numpy as jnp
from jax import lax
from jax.experimental import pallas as pl
from jax.experimental.pallas import tpu as pltpu
from jax.sharding import Mesh
from jax.sharding import PartitionSpec as P

STEP = 20
AXES = ("slab", "tile_0", "tile_1", "tile_2")
TILE = AXES[1:]

RENDER_WEIGHT = 1000.0
TV_WEIGHT = 0.05
BACKGROUND = 1.0
STEP_SPAN = 4.0
CLIP_RMS = 0.25
LEARN_RATE = 0.02
BETA_ONE = 0.9
BETA_TWO = 0.99
EPSILON = 1e-08

MESH_ID = pl.DeviceIdType.MESH
F32 = jnp.float32
BF16 = jnp.bfloat16
DEPTH = 16
ROWS = 8
WIDE = 256
KEYS = DEPTH * ROWS
CELLS = 4 * KEYS


def split_bf16(value):
    high = value.astype(BF16)
    return high, (value - high.astype(F32)).astype(BF16)


def sigmoid(value):
    return 1.0 / (1.0 + jnp.exp(-value))


def gradient_kernel(
    sizes,
    step_width,
    grid_hbm,
    first_hbm,
    second_hbm,
    pixel_hbm,
    start_hbm,
    count_hbm,
    target_hbm,
    grid,
    first,
    second,
    grad,
    total_ref,
    pixel,
    start,
    count,
    target,
    table,
    shade,
    clear,
    share,
    smooth,
    spread,
    columns,
    upright,
    chosens,
    rank,
    rank_half,
    edges,
    halo,
    out_part,
    in_part,
    out_cot,
    in_cot,
    mine,
    sums_a,
    sums_b,
    grid_sem,
    rays_sem,
    moment_sem,
    halo_sem,
    part_sem,
    cot_send,
    cot_recv,
    a_sem,
    b_sem,
    ready,
):
    slabs, size_x, size_y, cores = sizes
    group = pixel.shape[1] // slabs
    slab = lax.axis_index("slab")
    at_x = lax.axis_index("tile_0")
    at_y = lax.axis_index("tile_1")
    core = lax.axis_index("tile_2")
    tiles = size_x * size_y * cores
    tile = (at_x * size_y + at_y) * cores + core
    n_a = slabs * cores
    n_b = size_x * size_y
    lead = cores - 1
    leads = core == lead
    me_a = slab * cores + core
    me_b = at_x * size_y + at_y

    def remote(source, into, send, recv, device):
        return pltpu.make_async_remote_copy(
            src_ref=source,
            dst_ref=into,
            send_sem=send,
            recv_sem=recv,
            device_id=device,
            device_id_type=MESH_ID,
        )

    def signal(semaphore, device):
        pl.semaphore_signal(semaphore, inc=1, device_id=device, device_id_type=MESH_ID)

    def tile_device(index):
        return (slab, index // (size_y * cores), (index // cores) % size_y, index % cores)

    def far_first(size):
        return sorted(range(1, size), key=lambda off: -min(off, size - off))

    over_a = [(z, c) for z in far_first(slabs) + [0] for c in range(cores) if z or c]
    over_b = sorted(
        ((x, y) for x in range(size_x) for y in range(size_y) if x or y),
        key=lambda off: -min(off[0], size_x - off[0]) - min(off[1], size_y - off[1]),
    )

    def device_a(off):
        return ((slab + off[0]) % slabs, at_x, at_y, (core + off[1]) % cores)

    def device_b(off, at_core):
        return (slab, (at_x + off[0]) % size_x, (at_y + off[1]) % size_y, at_core)

    barrier = pltpu.get_barrier_semaphore()
    greet = [device_a(off) for off in over_a]
    assert size_y <= 8
    two_away = [y for y in far_first(size_y) if min(y, size_y - y) == 2] if size_y > 4 else []
    greet += [
        device_b((0, y), c)
        for y in far_first(size_y)
        if min(y, size_y - y) <= 2
        for c in range(cores)
    ]
    greet += [device_b((x, 0), core) for x in far_first(size_x)]
    next_tile = tile_device((tile + 1) % tiles)
    prev_tile = tile_device((tile + tiles - 1) % tiles)
    greet += [next_tile, prev_tile]

    load_grid = pltpu.make_async_copy(grid_hbm, grid, grid_sem)
    load_grid.start()
    for device in greet:
        signal(barrier, device)
    ray_loads = [
        pltpu.make_async_copy(source, into, rays_sem.at[k])
        for k, (source, into) in enumerate(
            ((pixel_hbm, pixel), (start_hbm, start), (count_hbm, count), (target_hbm, target))
        )
    ]
    for load in ray_loads:
        load.start()
    moment_loads = [
        pltpu.make_async_copy(first_hbm, first, moment_sem.at[0]),
        pltpu.make_async_copy(second_hbm, second, moment_sem.at[1]),
    ]

    row_at = lax.broadcasted_iota(jnp.int32, (ROWS, WIDE), 0)
    lane_at = lax.broadcasted_iota(jnp.int32, (ROWS, WIDE), 1)
    rank[...] = lax.broadcasted_iota(jnp.int32, (KEYS, 128), 0)
    rank_half[...] = lax.broadcasted_iota(jnp.int32, (WIDE, 128), 0).astype(F32).astype(BF16)

    spread[...] = jnp.zeros_like(spread)

    load_grid.wait()
    for load in moment_loads:
        load.start()
    light = jnp.ones((ROWS, WIDE), F32)
    color = [jnp.zeros((ROWS, WIDE), F32) for _ in range(3)]
    pairs = []
    for z in range(DEPTH):
        raw = grid[0, z]
        soft = jnp.maximum(raw, 0.0) + jnp.log(1.0 + jnp.exp(-jnp.abs(raw)))
        stay = jnp.exp(-(soft * step_width))
        weight = light * (1.0 - stay)
        light = light * stay
        share[z] = weight
        clear[z] = light
        for c in range(3):
            tone = sigmoid(grid[c + 1, z])
            shade[c, z] = tone
            color[c] = color[c] + weight * tone
        pairs.append((*color, 1.0 - light))
        if z % 2:
            for c in range(4):
                high, low = split_bf16(jnp.concatenate([pairs[-2][c], pairs[-1][c]], axis=0))
                at = c * KEYS + (z - 1) * ROWS
                table[pl.ds(at, 2 * ROWS), :] = high
                table[pl.ds(CELLS + at, 2 * ROWS), :] = low
    for load in ray_loads:
        load.wait()

    def partner(place):
        half = (place + 1) // 2
        return (slab + half * (2 * (place % 2) - 1) + slabs) % slabs

    def leader(other):
        return (other, at_x, at_y, lead)

    def packed_row(row):
        return jnp.broadcast_to(row.astype(F32), (16, group)).astype(BF16)

    def look_up(other):
        lanes = pl.ds(pl.multiple_of(other * group, group), group)
        cell = pixel[:, lanes]
        begin = start[:, lanes]
        taken = begin * DEPTH + count[:, lanes] - slab * DEPTH
        taken = jnp.where(begin <= slab, jnp.clip(taken, 0, DEPTH), 0)
        key = (taken - 1) * ROWS + lax.shift_right_logical(cell, 8)
        one = jnp.ones((16, 128), BF16)
        zero = jnp.zeros((16, 128), BF16)
        for ref, row, height in (
            (columns, packed_row(cell & (WIDE - 1)), WIDE),
            (chosens, packed_row(key), KEYS),
        ):
            for k in range(0, height, 16):
                level = rank_half[pl.ds(k, 16), :]
                for t in range(0, group, 128):
                    ref[other, pl.ds(k, 16), pl.ds(t, 128)] = jnp.where(
                        level == row[:, t : t + 128], one, zero
                    )
        rows = []
        for half in range(0, group, WIDE):
            found = jnp.dot(
                table[...], columns[other, :, pl.ds(half, WIDE)], preferred_element_type=F32
            )
            for t in range(0, WIDE, 128):
                wanted = jnp.broadcast_to(key[:, half + t : half + t + 128], (ROWS, 128))
                kept = [jnp.zeros((ROWS, 128), F32) for _ in range(4)]
                for k in range(0, KEYS, ROWS):
                    hit = rank[pl.ds(k, ROWS), :] == wanted
                    for c in range(4):
                        high, low = (
                            found[at + c * KEYS + k : at + c * KEYS + k + ROWS, t : t + 128]
                            for at in (0, CELLS)
                        )
                        kept[c] = jnp.where(hit, high + low, kept[c])
                rows.append([jnp.sum(keep, axis=0, keepdims=True) for keep in kept])
        values = [jnp.concatenate([row[c] for row in rows], axis=1) for c in range(4)]
        values[3] = 1.0 - values[3]
        return jnp.concatenate(values, axis=0)

    def send_part(slot, into, other):
        remote(
            out_part.at[slot], in_part.at[into], part_sem.at[0], part_sem.at[1], leader(other)
        ).start()

    places = list(range(slabs - 1, 0, -1))
    early = places[: slabs // 2]
    for place in early:
        out_part[partner(place)] = look_up(partner(place))
    pl.semaphore_wait(barrier, len(greet))
    for place in early:
        send_part(partner(place), me_a, partner(place))

    @pl.when(leads)
    def _():
        for y in two_away:
            signal(ready.at[0], device_b((0, y), lead))

    for place in places[slabs // 2 :]:
        out_part[partner(place)] = look_up(partner(place))
        send_part(partner(place), me_a, partner(place))
    out_part[slab] = look_up(slab)
    goal = target[:, pl.ds(pl.multiple_of(slab * group, group), group)]

    @pl.when(jnp.logical_not(leads))
    def _():
        send_part(slab, me_a, slab)
        out_part[slabs] = jnp.concatenate([goal, jnp.zeros((1, group), F32)], axis=0)
        send_part(slabs, n_a, slab)

    for c in range(4):
        for z in range(DEPTH):
            k = c * DEPTH + z
            edges[0, k // ROWS, pl.ds(k % ROWS, 1), :] = grid[c, z, pl.ds(ROWS - 1, 1), :]
            edges[1, k // ROWS, pl.ds(k % ROWS, 1), :] = grid[c, z, pl.ds(0, 1), :]
    for source, into, device in (
        (edges.at[0], halo.at[pl.ds(8, 8)], next_tile),
        (edges.at[1], halo.at[pl.ds(16, 8)], prev_tile),
        (grid.at[:, DEPTH - 1], halo.at[pl.ds(0, 4)], device_a((1, 0))),
        (grid.at[:, 0], halo.at[pl.ds(4, 4)], device_a((slabs - 1, 0))),
    ):
        remote(source, into, halo_sem.at[0], halo_sem.at[1], device).start()

    def stand_up(other, carry):
        cell = pixel[:, pl.ds(pl.multiple_of(other * group, group), group)]
        column = (cell & (WIDE - 1)).astype(F32)
        level = lax.broadcasted_iota(jnp.int32, (16, WIDE), 1).astype(F32).astype(BF16)
        one = jnp.ones((16, WIDE), BF16)
        zero = jnp.zeros((16, WIDE), BF16)
        for t in range(0, group, 128):
            down = jnp.broadcast_to(column[:, t : t + 128], (128, 128)).T.astype(BF16)
            for k in range(0, 128, 16):
                tall = down[k : k + 16]
                upright[other, pl.ds(t + k, 16), :] = jnp.where(
                    jnp.concatenate([tall] * (WIDE // 128), axis=1) == level, one, zero
                )
        return carry

    lax.fori_loop(0, slabs, stand_up, 0)

    def part_blocks(n):
        part = in_part.at[pl.ds(0, n)]
        return remote(part, part, part_sem.at[0], part_sem.at[1], next_tile)

    def cot_blocks(n, slot):
        cot = out_cot.at[pl.ds(0, n)]
        return remote(cot, cot, cot_send, cot_recv.at[slot], next_tile)

    @pl.when(leads)
    def _():
        in_part[me_a] = out_part[slab]
        part_blocks(n_a).wait_recv()
        for c in range(cores):
            ahead = jnp.ones((1, group), F32)
            rendered = jnp.zeros((3, group), F32)
            reach = []
            for s in range(slabs):
                reach.append(ahead)
                part = in_part[s * cores + c]
                rendered = rendered + ahead * part[:3]
                ahead = ahead * part[3:]
            wish = goal if c == lead else in_part[n_a][:3]
            residual = RENDER_WEIGHT * (rendered + ahead * BACKGROUND - wish)
            beyond = jnp.full((3, group), BACKGROUND, F32)
            for s in range(slabs - 1, -1, -1):
                product = residual * beyond
                dark = product[0:1] + product[1:2] + product[2:3]
                out_cot[s * cores + c] = reach[s] * jnp.concatenate([residual, dark], axis=0)
                part = in_part[s * cores + c]
                beyond = part[:3] + part[3:] * beyond
        for place in range(slabs):
            other = partner(place)
            for c in range(cores):
                if place or c != lead:
                    remote(
                        out_cot.at[other * cores + c],
                        in_cot.at[slab],
                        cot_send,
                        cot_recv.at[slab],
                        (other, at_x, at_y, c),
                    ).start()
        in_cot[slab] = out_cot[slab * cores + lead]

    def scatter(other):
        high, low = split_bf16(in_cot[other])
        chosen = chosens[other]
        left = jnp.concatenate(
            [chosen * half[c : c + 1] for half in (high, low) for c in range(4)], axis=0
        )
        found = jnp.dot(left, upright[other], preferred_element_type=F32)
        return found[:CELLS] + found[CELLS:]

    remote(halo, halo, halo_sem.at[0], halo_sem.at[1], next_tile).wait()

    def smooth_channel(c, carry):
        for z in range(DEPTH):
            value = grid[c, z]
            if z > 0:
                total = value - grid[c, z - 1]
            else:
                total = jnp.where(slab > 0, value - halo[c], 0.0)
            if z < DEPTH - 1:
                total += value - grid[c, z + 1]
            else:
                total += jnp.where(slab < slabs - 1, value - halo[4 + c], 0.0)
            line = (2 * c + z // ROWS, pl.ds(z % ROWS, 1), slice(None))
            below = jnp.where(
                row_at == 0, halo[8 + line[0], line[1], line[2]], pltpu.roll(value, 1, 0)
            )
            above = jnp.where(
                row_at == ROWS - 1,
                halo[16 + line[0], line[1], line[2]],
                pltpu.roll(value, ROWS - 1, 0),
            )
            total += jnp.where((row_at > 0) | (tile > 0), value - below, 0.0)
            total += jnp.where((row_at < ROWS - 1) | (tile < tiles - 1), value - above, 0.0)
            total += jnp.where(lane_at > 0, value - pltpu.roll(value, 1, 1), 0.0)
            total += jnp.where(lane_at < WIDE - 1, value - pltpu.roll(value, WIDE - 1, 1), 0.0)
            smooth[c, z] = (2.0 * TV_WEIGHT) * total
        return carry

    lax.fori_loop(0, 4, smooth_channel, 0)

    @pl.when(leads)
    def _():
        if two_away:
            pl.semaphore_wait(ready.at[0], len(two_away))
        for x in far_first(size_x):
            signal(ready.at[1], device_b((x, 0), lead))


    def scatter_arrived(place, carry):
        other = partner(place)

        @pl.when((place > 0) | jnp.logical_not(leads))
        def _():
            cot_blocks(1, other).wait_recv()

        spread[...] += scatter(other)
        return carry

    lax.fori_loop(0, slabs, scatter_arrived, 0)

    later = [jnp.zeros((ROWS, WIDE), F32) for _ in range(3)]
    tail = jnp.zeros((ROWS, WIDE), F32)
    squares = jnp.zeros((ROWS, WIDE), F32)
    for z in range(DEPTH - 1, -1, -1):
        weight = share[z]
        light = clear[z]
        pull = jnp.zeros((ROWS, WIDE), F32)
        for c in range(3):
            tone = shade[c, z]
            later[c] = later[c] + spread[pl.ds(c * KEYS + z * ROWS, ROWS), :]
            pull = pull + tone * later[c]
            value = weight * later[c] * (tone * (1.0 - tone)) + smooth[c + 1, z]
            grad[c + 1, z] = value
            squares = squares + value * value
        tail = tail + spread[pl.ds(3 * KEYS + z * ROWS, ROWS), :] * light
        thick = pull * light - tail
        tail = tail + pull * weight
        value = thick * (step_width * sigmoid(grid[0, z])) + smooth[0, z]
        grad[0, z] = value
        squares = squares + value * value

    squares = squares[:, :128] + squares[:, 128:]
    own = jnp.sum(squares, axis=0, keepdims=True)
    mine[0] = own

    def send_a(other):
        remote(mine.at[0], sums_a.at[me_a], a_sem.at[0], a_sem.at[1], leader(other)).start()

    def blocks(sums, n, send, recv):
        some = sums.at[pl.ds(0, n)]
        return remote(some, some, send, recv, next_tile)

    for off in far_first(slabs):
        send_a((slab + off) % slabs)

    @pl.when(jnp.logical_not(leads))
    def _():
        send_a(slab)
        part_blocks(slabs + 1).wait_send()
        blocks(sums_a, slabs, a_sem.at[0], a_sem.at[1]).wait_send()
        for load in moment_loads:
            load.wait()
        blocks(sums_b, n_b, b_sem.at[0], b_sem.at[2]).wait_recv()

    @pl.when(leads)
    def _():
        sums_a[me_a] = own
        part_blocks(slabs - 1).wait_send()
        cot_blocks(n_a - 1, 0).wait_send()
        for load in moment_loads:
            load.wait()
        if size_x > 1:
            pl.semaphore_wait(ready.at[1], size_x - 1)
        blocks(sums_a, n_a - 1, a_sem.at[0], a_sem.at[1]).wait_recv()
        share_b = jnp.sum(sums_a[...], axis=0)
        mine[1] = share_b
        for off in over_b + [(0, 0)]:
            for c in range(cores):
                if off != (0, 0) or c != lead:
                    remote(
                        mine.at[1],
                        sums_b.at[me_b],
                        b_sem.at[1 if c == lead else 0],
                        b_sem.at[2],
                        device_b(off, c),
                    ).start()
        sums_b[me_b] = share_b
        blocks(sums_a, slabs - 1, a_sem.at[0], a_sem.at[1]).wait_send()
        blocks(sums_b, n_b, b_sem.at[0], b_sem.at[2]).wait_send()
        if n_b > 1:
            blocks(sums_b, n_b - 1, b_sem.at[1], b_sem.at[2]).wait()

    total_ref[...] = jnp.sum(sums_b[...], axis=0)


def update_kernel(limit, grid, first, second, grad, total, *rest):
    outs, held, sem = rest[:3], rest[3:6], rest[6]
    norm = jnp.sqrt(jnp.sum(total[...], axis=1, keepdims=True))
    scale = jnp.broadcast_to(limit / jnp.maximum(norm, limit), (ROWS, WIDE))
    rate = LEARN_RATE / (1.0 - BETA_ONE**STEP)
    for c in range(4):
        for z in range(DEPTH):
            clipped = grad[c, z] * scale
            new_first = BETA_ONE * first[c, z] + (1.0 - BETA_ONE) * clipped
            new_second = BETA_TWO * second[c, z] + ((1.0 - BETA_TWO) * clipped) * clipped
            second_hat = new_second * (1.0 / (1.0 - BETA_TWO**STEP))
            root = second_hat * lax.rsqrt(second_hat)
            held[0][c, z] = grid[c, z] - (rate * new_first) * pl.reciprocal(root + EPSILON)
            held[1][c, z] = new_first
            held[2][c, z] = new_second
            if z % 4 == 3:
                for k in range(3):
                    part = (c, pl.ds(z - 3, 4))
                    pltpu.make_async_copy(
                        held[k].at[part], outs[k].at[part], sem.at[k]
                    ).start()
    for k in range(3):
        pltpu.make_async_copy(held[k], outs[k], sem.at[k]).wait()


def per_device(voxel_grid, first_moment, second_moment, pixel_index, start_slab, ray_count, target):
    sizes = tuple(lax.axis_size(axis) for axis in AXES)
    slabs = sizes[0]
    rays = pixel_index.shape[0]
    group = rays // slabs
    total_depth = DEPTH * slabs
    total_x = ROWS * math.prod(sizes[1:])
    n_a = slabs * sizes[3]
    n_b = sizes[1] * sizes[2]
    block = (4, DEPTH, ROWS, WIDE)
    dma = pltpu.SemaphoreType.DMA
    anywhere = pl.BlockSpec(memory_space=pl.ANY)
    inside = pl.BlockSpec(memory_space=pltpu.VMEM)
    held = pltpu.VMEM(block, F32)
    grid, first, second, grad, total = pl.pallas_call(
        functools.partial(gradient_kernel, sizes, STEP_SPAN / total_depth),
        out_shape=(held, held, held, held, pltpu.VMEM((1, 128), F32)),
        in_specs=[anywhere] * 7,
        out_specs=(inside,) * 5,
        scratch_shapes=[
            pltpu.VMEM((1, rays), jnp.int32),
            pltpu.VMEM((1, rays), jnp.int32),
            pltpu.VMEM((1, rays), jnp.int32),
            pltpu.VMEM((3, rays), F32),
            pltpu.VMEM((2 * CELLS, WIDE), BF16),
            pltpu.VMEM((3, DEPTH, ROWS, WIDE), F32),
            pltpu.VMEM((DEPTH, ROWS, WIDE), F32),
            pltpu.VMEM((DEPTH, ROWS, WIDE), F32),
            pltpu.VMEM(block, F32),
            pltpu.VMEM((CELLS, WIDE), F32),
            pltpu.VMEM((slabs, WIDE, group), BF16),
            pltpu.VMEM((slabs, group, WIDE), BF16),
            pltpu.VMEM((slabs, KEYS, group), BF16),
            pltpu.VMEM((KEYS, 128), jnp.int32),
            pltpu.VMEM((WIDE, 128), BF16),
            pltpu.VMEM((2, 8, ROWS, WIDE), F32),
            pltpu.VMEM((24, ROWS, WIDE), F32),
            pltpu.VMEM((slabs + 1, 4, group), F32),
            pltpu.VMEM((n_a + 1, 4, group), F32),
            pltpu.VMEM((n_a, 4, group), F32),
            pltpu.VMEM((slabs, 4, group), F32),
            pltpu.VMEM((2, 1, 128), F32),
            pltpu.VMEM((n_a, 1, 128), F32),
            pltpu.VMEM((n_b, 1, 128), F32),
            dma,
            dma((4,)),
            dma((2,)),
            dma((2,)),
            dma((2,)),
            dma,
            dma((slabs,)),
            dma((2,)),
            dma((3,)),
            pltpu.SemaphoreType.REGULAR((2,)),
        ],
        compiler_params=pltpu.CompilerParams(collective_id=0, has_side_effects=True),
        name="render_gradient",
    )(
        voxel_grid,
        first_moment,
        second_moment,
        pixel_index.reshape(1, rays),
        start_slab.reshape(1, rays),
        ray_count.reshape(1, rays),
        target,
    )
    limit = CLIP_RMS * math.sqrt(4.0 * total_depth * total_x * WIDE)
    return pl.pallas_call(
        functools.partial(update_kernel, limit),
        out_shape=[jax.ShapeDtypeStruct(block, F32)] * 3,
        in_specs=[inside] * 5,
        out_specs=[anywhere] * 3,
        scratch_shapes=[held, held, held, dma((3,))],
        compiler_params=pltpu.CompilerParams(vmem_limit_bytes=16 * 2**20),
        name="clipped_adam",
    )(grid, first, second, grad, total)


def solution(mesh):
    torus = Mesh(mesh.devices.reshape(mesh.shape["slab"], 4, 8, 2), AXES)
    cells = P(None, "slab", TILE, None)
    rays = P(TILE)
    return jax.shard_map(
        per_device,
        mesh=torus,
        in_specs=(cells, cells, cells, rays, rays, rays, P(None, TILE)),
        out_specs=(cells, cells, cells),
        check_vma=False,
    )
```
